32 devices in a mesh: comp: 2 (over core), tgt: 4 (over y, x), src: 4 (over z).
Axes of the slice: x: 2, y: 2, z: 4, core: 2. Of those that a mesh axis runs over, the one named last changes fastest.
Arguments:
- field: bfloat16 [3, 32, 8192], P(None, None, ('tgt', 'src')), may hold values from -6 to 6
- dest_group: int32 [4096, 1], P(('comp', 'tgt', 'src')), may hold values from 0 to 3; in each aligned block of 128 rows (0 to 127, 128 to 255, ...) at most 64 rows name the same one
- src_local: int32 [4096], P(('comp', 'tgt', 'src')), may hold values from 0 to 1
- ranks: int32 [4096], P(('comp', 'tgt', 'src')), may hold values from 8 to 64
- mixing: float32 [4096, 3, 3], P(('comp', 'tgt', 'src')), may hold values from -5 to 5
- v_factor: bfloat16 [4096, 64, 256], P(('comp', 'tgt', 'src')), may hold values from -0.375 to 0.375
- u_factor: bfloat16 [8192, 64, 256], P(('comp', 'tgt', 'src')), may hold values from -0.0625 to 0.0625
- slot_cluster: int32 [8192], P(('comp', 'tgt', 'src')), may hold values from 0 to 7
- near_src: int32 [128], P(('comp', 'tgt', 'src')), may hold values from 0 to 1
- near_tgt: int32 [128], P(('comp', 'tgt', 'src')), may hold values from 0 to 7
- near_mixing: float32 [128, 3, 3], P(('comp', 'tgt', 'src')), may hold values from -5 to 5
- near_matrix: bfloat16 [128, 256, 256], P(('comp', 'tgt', 'src')), may hold values from -0.1875 to 0.1875
Outputs:
- result: float32 [3, 32, 8192], P(None, None, ('comp', 'tgt', 'src'))
The draws below stay inside these ranges and needn't reach their ends.
Inputs may be any that keep to these rules, and one draw needn't show every extreme that they name: `dest_group`: among the 128 blocks of one device at most 64 name the same target group, and in every draw some device has exactly 64 blocks to one group.
All inputs are finite; a program needn't handle non-finite values.
Results may differ from the reference program's by a relative error of at most 0.0018.
Values may be sent and summed in bfloat16 or wider, within the bound.
A program may use at most 128 MiB of HBM per device.

```python
import math
import jax
import jax.numpy as jnp
import numpy as np
from jax import lax

CL = 256
R = 64
RHS = 32
CLU_DEV = 2
BLK_DEV = 128
NEAR_DEV = 4
CAP = 64
NPTS = 8192
NBLK = 4096
USLOTS = 8192
NNEAR = 128
N_COMP = 2
N_TGT = 4
N_SRC = 4


def touch_ends(drawn, key, least, largest):
    longest = drawn.shape.index(max(drawn.shape))
    spots = []
    for shift in (0, 1):
        where = [jax.random.randint(jax.random.fold_in(key, axis), (), 0, length) for axis, length in enumerate(drawn.shape)]
        where[longest] = (where[longest] + shift) % drawn.shape[longest]
        spots.append(tuple(where))
    return drawn.at[spots[0]].set(least).at[spots[1]].set(largest)


def steps_of(own_key, dims, shards, smallest, largest):
    level = 1.0
    for axis_at, shards_of in shards:
        steps = jax.random.uniform(jax.random.fold_in(jax.random.fold_in(own_key, 6), axis_at), (shards_of,), jnp.float32, smallest / len(shards), largest / len(shards))
        level = level * jnp.repeat(jnp.exp(steps), dims[axis_at] // shards_of).reshape((-1,) + (1,) * (len(dims) - 1 - axis_at))
    return level


def assign_block(own_key, own, number, rows, count, top, reach, skew):
    order = jax.random.permutation(own_key, count)
    crowded, usual = load_shares(count, rows * top, reach, skew, True), load_shares(count, rows * top, reach, skew, False)
    places = jnp.arange(count)

    def named(sizes, offset_by):
        used = int((sizes > 0).sum())
        fixed = max(1, used // 4)
        shifted = fixed + (places - fixed + offset_by * (used - fixed)) % max(1, count - fixed)
        return jnp.zeros((count,), jnp.int32).at[order[jnp.where(places < fixed, places, shifted)]].set(jnp.asarray(sizes, jnp.int32))

    sizes = jnp.where(number % 4 == 0, named(crowded, number // 4), named(usual, number - number // 4 - 1))
    mixed = jax.random.permutation(jax.random.fold_in(own, 3), count)
    donor, taker = mixed[0:count // 2 * 2:2], mixed[1:count // 2 * 2:2]
    room = jnp.minimum(sizes[donor] - 1, reach - sizes[taker]) // 2
    room = jnp.where((donor == order[0]) | (taker == order[0]) | (sizes[taker] == 0), 0, jnp.maximum(room, 0))
    shifted = jax.random.randint(jax.random.fold_in(own, 4), (count // 2,), 0, 1 << 20) % (room + 1)
    sizes = sizes.at[donor].add(-shifted).at[taker].add(shifted)
    members = jnp.searchsorted(jnp.cumsum(sizes), jnp.arange(rows * top), side="right").astype(jnp.int32)
    grid = members.reshape(top, rows).T
    grid = grid[jax.random.permutation(jax.random.fold_in(own, 1), rows)]
    offset_by = jax.random.randint(jax.random.fold_in(own, 2), (rows, 1), 0, top)
    return jnp.take_along_axis(grid, (jnp.arange(top)[None, :] + offset_by) % top, axis=1)


def load_shares(count, total, most, lean, full):
    portions = [(1 << 20) // math.isqrt(standing ** lean) + 1 for standing in range(1, count + 1)]
    largest = most if full else min(most, max(-(-total // count), total * portions[0] // sum(portions)))
    least = 1 if total - largest >= count - 1 else 0
    counts, surplus = [largest] + [least] * (count - 1), total - largest - least * (count - 1)
    while surplus > 0:
        candidates = [i for i in range(1, count) if counts[i] < largest] or [i for i in range(1, count) if counts[i] < most]
        whole, left = sum([portions[i] for i in candidates]), surplus
        for i in candidates:
            addition = min(most - counts[i], max(1, left * portions[i] // whole), surplus)
            counts[i] = counts[i] + addition
            surplus = surplus - addition
    return np.array(counts)


def noise(own_key, extent, scale, reach, shards=(), kind=jnp.bfloat16):
    loudness = steps_of(own_key, extent, shards, -0.22, 0.18) if shards else 1.0
    values = jax.random.normal(own_key, extent, jnp.float32) * scale * loudness
    return jnp.minimum(jnp.maximum(values, -reach), reach).astype(kind)


def setup_inputs(seed: int = 0) -> dict:
    streams_of = jax.random.split(jax.random.key(seed), 13)
    field = noise(streams_of[0], (3, RHS, NPTS), 1.0, 6.0, ((2, 16),))
    dest_group_keys = jax.random.split(jax.random.fold_in(streams_of[1], 1), NBLK // BLK_DEV)
    dest_group_turns = jax.random.permutation(jax.random.fold_in(streams_of[1], 3), NBLK // BLK_DEV)
    dest_group = jax.vmap(lambda own, number: assign_block(jax.random.fold_in(streams_of[1], 2), own, number, BLK_DEV, N_TGT, 1, CAP, 2))(dest_group_keys, dest_group_turns).reshape((NBLK, 1))
    src_local = touch_ends(jax.random.randint(streams_of[2], (NBLK,), 0, CLU_DEV), jax.random.fold_in(streams_of[2], 1), 0, CLU_DEV - 1).astype(jnp.int32)
    ranks = touch_ends(jax.random.randint(streams_of[3], (NBLK,), max(1, R // 8), R + 1), jax.random.fold_in(streams_of[3], 1), max(1, R // 8), R).astype(jnp.int32)
    mixing = noise(streams_of[4], (NBLK, 3, 3), 1.0, 5.0, ((0, 32),), jnp.float32)
    v_factor = noise(streams_of[5], (NBLK, R, CL), CL ** -0.5, 0.375, ((0, 32),))
    u_factor = noise(streams_of[6], (USLOTS, R, CL), (R * BLK_DEV) ** -0.5, 0.0625, ((0, 32),))
    slot_cluster = touch_ends(jax.random.randint(streams_of[7], (USLOTS,), 0, CLU_DEV * N_SRC), jax.random.fold_in(streams_of[7], 1), 0, (CLU_DEV * N_SRC) - 1).astype(jnp.int32)
    near_src = touch_ends(jax.random.randint(streams_of[8], (NNEAR,), 0, CLU_DEV), jax.random.fold_in(streams_of[8], 1), 0, CLU_DEV - 1).astype(jnp.int32)
    near_tgt = touch_ends(jax.random.randint(streams_of[9], (NNEAR,), 0, CLU_DEV * N_SRC), jax.random.fold_in(streams_of[9], 1), 0, (CLU_DEV * N_SRC) - 1).astype(jnp.int32)
    near_mixing = noise(streams_of[10], (NNEAR, 3, 3), 1.0, 5.0, ((0, 32),), jnp.float32)
    near_matrix = noise(streams_of[11], (NNEAR, CL, CL), (CL * NEAR_DEV) ** -0.5, 0.1875, ((0, 32),))
    return dict(field=field, dest_group=dest_group, src_local=src_local, ranks=ranks, mixing=mixing, v_factor=v_factor, u_factor=u_factor, slot_cluster=slot_cluster, near_src=near_src, near_tgt=near_tgt, near_mixing=near_mixing, near_matrix=near_matrix)


def reference(field, dest_group, src_local, ranks, mixing, v_factor, u_factor, slot_cluster, near_src, near_tgt, near_mixing, near_matrix):
    devices = N_COMP * N_TGT * N_SRC
    channels = 3 * RHS
    half_owned = CLU_DEV // 2
    source_count = N_TGT * N_SRC * CLU_DEV
    sources = jnp.transpose(field.reshape(channels, source_count, CL), (1, 0, 2))
    device_ids = jnp.arange(devices, dtype=jnp.int32)
    comp_of = device_ids // (N_TGT * N_SRC)
    tgt_of = (device_ids // N_SRC) % N_TGT
    src_of = device_ids % N_SRC
    destination = dest_group.reshape(devices, BLK_DEV).astype(jnp.int32)
    member = (destination[:, :, None] == jnp.arange(N_TGT, dtype=jnp.int32)[None, None, :]).astype(jnp.int32)
    position = jnp.sum(jnp.cumsum(member, axis=1) * member, axis=2) - 1
    sender_row = tgt_of * N_SRC + src_of
    source_ids = sender_row[:, None] * CLU_DEV + src_local.reshape(devices, BLK_DEV)
    receiver = (comp_of[:, None] * N_TGT + destination) * N_SRC + src_of[:, None]
    u_rows = (receiver * (N_TGT * CAP) + tgt_of[:, None] * CAP + position).astype(jnp.int32)
    within = slot_cluster[u_rows.reshape(-1)].reshape(devices, BLK_DEV)

    def global_target(group, inner):
        comp_part = inner // (N_SRC * half_owned)
        src_part = (inner // half_owned) % N_SRC
        local_part = inner % half_owned
        return (((comp_part * N_TGT + group) * N_SRC + src_part) * half_owned + local_part).astype(jnp.int32)

    far_targets = global_target(destination, within)
    near_targets = global_target(jnp.broadcast_to(tgt_of[:, None], (devices, NEAR_DEV)), near_tgt.reshape(devices, NEAR_DEV))
    near_sources = sender_row[:, None] * CLU_DEV + near_src.reshape(devices, NEAR_DEV)
    total = jnp.zeros((N_COMP * N_TGT * N_SRC * half_owned, channels, CL), jnp.float32)

    def far_step(carry, items):
        source_rows, rank_row, mix_row, v_rows, u_index, target_rows = items
        inputs = sources[source_rows].astype(jnp.float32)
        coefficients = jnp.einsum("bfp,brp->bfr", inputs, v_rows.astype(jnp.float32))
        rank_mask = (jnp.arange(R, dtype=jnp.int32)[None, :] < rank_row[:, None]).astype(jnp.float32)
        coefficients = (coefficients * rank_mask[:, None, :]).reshape(BLK_DEV, 3, RHS, R)
        mixed_coef = jnp.einsum("bcd,bdsr->bcsr", mix_row.astype(jnp.float32), coefficients)
        sent = lax.optimization_barrier(mixed_coef.reshape(BLK_DEV, channels, R).astype(jnp.bfloat16))
        basis = u_factor[u_index].astype(jnp.float32)
        contrib = jnp.einsum("bfr,brq->bfq", sent.astype(jnp.float32), basis)
        return carry.at[target_rows].add(contrib), None

    total, unused = lax.scan(far_step, total, (source_ids, ranks.reshape(devices, BLK_DEV), mixing.reshape(devices, BLK_DEV, 3, 3), v_factor.reshape(devices, BLK_DEV, R, CL), u_rows, far_targets))

    def near_step(carry, items):
        source_rows, mix_row, dense_rows, target_rows = items
        inputs = sources[source_rows].astype(jnp.float32)
        dense_out = jnp.einsum("nfp,nqp->nfq", inputs, dense_rows.astype(jnp.float32)).reshape(NEAR_DEV, 3, RHS, CL)
        mixed_near = jnp.einsum("ncd,ndsq->ncsq", mix_row.astype(jnp.float32), dense_out).reshape(NEAR_DEV, channels, CL)
        return carry.at[target_rows].add(mixed_near), None

    total, unused = lax.scan(near_step, total, (near_sources, near_mixing.reshape(devices, NEAR_DEV, 3, 3), near_matrix.reshape(devices, NEAR_DEV, CL, CL), near_targets))
    return jnp.transpose(total, (1, 0, 2)).reshape(3, RHS, NPTS)
```

```python
import functools

import jax
import jax.numpy as jnp
from jax import lax
from jax.experimental import pallas as pl
from jax.experimental.pallas import tpu as pltpu
from jax.sharding import PartitionSpec as P

NT = (((1,), (1,)), ((), ()))
MESH = pl.DeviceIdType.MESH
HALVES = 2


def mix_rows(weights, parts):
    mixed = []
    for row in weights:
        total = row[0] * parts[0]
        for weight, part in zip(row[1:], parts[1:]):
            total = total + weight * part
        mixed.append(total)
    return mixed


def fused_kernel(
    sizes,
    field_hbm,
    dest_hbm,
    src_hbm,
    ranks_hbm,
    mix_ref,
    v_hbm,
    u_hbm,
    cluster,
    near_src,
    near_tgt,
    near_mix,
    near_hbm,
    out_ref,
    field_ref,
    x_ref,
    v_ref,
    u_ref,
    near_ref,
    rows_ref,
    meta_ref,
    meta,
    near_out,
    sent,
    got,
    lhs,
    acc,
    comp_got,
    total,
    cast,
    src_got,
    load_sem,
    u_sem,
    meta_sem,
    send_sem,
    recv_sem,
    comp_send,
    comp_recv,
    src_send,
    src_recv,
):
    groups, shards, pairing, components, chunk = sizes
    me = lax.axis_index("tgt")
    row = lax.axis_index("src")
    half_of = lax.axis_index("comp")
    owned, channels, size = x_ref.shape
    vectors = channels // components
    strip = vectors // HALVES
    band = components * strip
    slots, rank_width = u_hbm.shape[0] * 2, u_hbm.shape[1] // 2
    blocks = v_hbm.shape[0]
    capacity = slots // groups
    pairs = capacity // 2
    lanes = 2 * rank_width
    chunks = pairs // chunk
    targets = acc.shape[1] // band
    kept = targets // (pairing * shards)

    def load(index, source, target):
        return pltpu.make_async_copy(source, target, load_sem.at[index])

    small = [
        load(0, dest_hbm, rows_ref.at[0]),
        load(1, ranks_hbm, rows_ref.at[1]),
        load(2, src_hbm, rows_ref.at[2]),
    ]
    large = [load(3, field_hbm, field_ref), load(4, near_hbm, near_ref)]
    split = 4 if blocks % 4 == 0 else 1
    part = blocks // split
    v_loads = [
        load(5 + i, v_hbm.at[pl.ds(i * part, part)], v_ref.at[pl.ds(i * part, part)])
        for i in range(split)
    ]
    u_loads = [
        pltpu.make_async_copy(
            u_hbm.at[pl.ds(g * pairs, pairs)], u_ref.at[pl.ds(g * pairs, pairs)], u_sem.at[g]
        )
        for g in range(groups)
    ]
    for copy in small + large[:1] + v_loads + large[1:] + u_loads:
        copy.start()

    barrier = pltpu.get_barrier_semaphore()
    for step in range(1, groups):
        pl.semaphore_signal(
            barrier, inc=1, device_id={"tgt": jnp.bitwise_xor(me, step)}, device_id_type=MESH
        )
    for step in range(1, shards):
        pl.semaphore_signal(
            barrier, inc=1, device_id={"src": lax.rem(row + step, shards)}, device_id_type=MESH
        )
    for step in range(1, pairing):
        pl.semaphore_signal(
            barrier, inc=1, device_id={"comp": lax.rem(half_of + step, pairing)}, device_id_type=MESH
        )

    for copy in small:
        copy.wait()
    dest = rows_ref[0]
    padded = -(-groups // 16) * 16
    member = jnp.where(
        lax.broadcasted_iota(jnp.int32, (padded, blocks), 0) == dest, 1.0, 0.0
    )
    before = jnp.where(
        lax.broadcasted_iota(jnp.int32, (blocks, blocks), 0)
        < lax.broadcasted_iota(jnp.int32, (blocks, blocks), 1),
        1.0,
        0.0,
    ).astype(jnp.bfloat16)
    earlier = jnp.dot(member.astype(jnp.bfloat16), before, preferred_element_type=jnp.float32)
    position = jnp.sum(member * earlier, axis=0, keepdims=True)
    slot = dest * capacity + position.astype(jnp.int32)
    taken = jnp.where(
        lax.broadcasted_iota(jnp.int32, (slots, blocks), 0) == slot, 1.0, 0.0
    ).astype(jnp.bfloat16)
    line = lax.broadcasted_iota(jnp.int32, (16, blocks), 0)
    facts = jnp.where(
        line == 0,
        lax.broadcasted_iota(jnp.int32, (16, blocks), 1),
        jnp.where(line == 1, rows_ref[1], rows_ref[2]),
    )
    placed = lax.dot_general(
        facts.astype(jnp.float32).astype(jnp.bfloat16), taken, NT, preferred_element_type=jnp.float32
    )
    meta_ref[...] = placed[:8].astype(jnp.int32)
    to_scalars = pltpu.make_async_copy(meta_ref, meta, meta_sem)
    to_scalars.start()

    large[0].wait()
    for s in range(owned):
        x_ref[s] = field_ref[:, s * size : (s + 1) * size]
    to_scalars.wait()
    for copy in v_loads:
        copy.wait()

    lane = lax.broadcasted_iota(jnp.int32, (1, lanes), 1)
    first = lane < rank_width
    rank_at = lane % rank_width
    unroll = 4 if chunk % 4 == 0 else 1

    def coef_step(offset, start):
        base = jnp.bitwise_xor(me, offset) * capacity + 2 * start
        numbers = [jnp.clip(meta[0, base + i], 0, blocks - 1) for i in range(2 * unroll)]
        v = jnp.concatenate([v_ref[b] for b in numbers], axis=0)
        x = x_ref[...].reshape(owned * channels, size)
        y = lax.dot_general(x, v, NT, preferred_element_type=jnp.float32)
        for u in range(unroll):
            b0, b1 = numbers[2 * u], numbers[2 * u + 1]
            k0, k1 = base + 2 * u, base + 2 * u + 1
            here = y[:, u * lanes : (u + 1) * lanes]
            chosen = jnp.where(first, meta[2, k0], meta[2, k1])
            coef = here[:channels]
            for s in range(1, owned):
                coef = jnp.where(chosen == s, here[s * channels : (s + 1) * channels], coef)
            coef = jnp.where(rank_at < jnp.where(first, meta[1, k0], meta[1, k1]), coef, 0.0)
            weights = [
                [jnp.where(first, mix_ref[c, d, b0], mix_ref[c, d, b1]) for d in range(components)]
                for c in range(components)
            ]
            mixed = mix_rows(
                weights, [coef[d * vectors : (d + 1) * vectors] for d in range(components)]
            )
            for h in range(HALVES):
                for c in range(components):
                    sent[offset, h, start + u, c * strip : (c + 1) * strip, :] = mixed[c][
                        h * strip : (h + 1) * strip
                    ].astype(jnp.bfloat16)

    def coef_chunk(offset, c):
        def several(step, carry):
            coef_step(offset, c * chunk + step * unroll)
            return carry

        lax.fori_loop(0, chunk // unroll, several, 0)

    def exchange(offset, h, c):
        where = (h, pl.ds(c * chunk, chunk))
        return pltpu.make_async_remote_copy(
            src_ref=sent.at[(offset,) + where],
            dst_ref=got.at[(offset - 1,) + where],
            send_sem=send_sem.at[h, offset - 1, c],
            recv_sem=recv_sem.at[h, offset - 1, c],
            device_id={"tgt": jnp.bitwise_xor(me, offset)},
            device_id_type=MESH,
        )

    def over_offsets(action):
        def step(t, carry):
            action(groups - 1 - t)
            return carry

        lax.fori_loop(0, groups - 1, step, 0)

    def over_chunks(action):
        def step(c, carry):
            action(c)
            return carry

        lax.fori_loop(0, chunks, step, 0)

    pl.semaphore_wait(barrier, groups + shards + pairing - 3)

    def send_first(c):
        def one(offset):
            coef_chunk(offset, c)
            exchange(offset, 0, c).start()

        over_offsets(one)

    over_chunks(send_first)
    for h in range(1, HALVES):
        over_chunks(lambda c, h=h: over_offsets(lambda offset: exchange(offset, h, c).start()))
    over_chunks(lambda c: coef_chunk(0, c))

    large[1].wait()
    for n in range(near_ref.shape[0]):
        y = lax.dot_general(
            x_ref[near_src[n]], near_ref[n], NT, preferred_element_type=jnp.float32
        )
        weights = [[near_mix[c, n, d] for d in range(components)] for c in range(components)]
        mixed = mix_rows(weights, [y[d * vectors : (d + 1) * vectors] for d in range(components)])
        for h in range(HALVES):
            for c in range(components):
                near_out[h, n, c * strip : (c + 1) * strip, :] = mixed[c][
                    h * strip : (h + 1) * strip
                ]

    def place_near(w, carry):
        for h in range(HALVES):
            value = jnp.where(near_tgt[0] == w, near_out[h, 0], 0.0)
            for n in range(1, near_ref.shape[0]):
                value = value + jnp.where(near_tgt[n] == w, near_out[h, n], 0.0)
            acc[h, pl.ds(pl.multiple_of(w * band, band), band), :] = value
        return carry

    lax.fori_loop(0, targets, place_near, 0)
    for copy in u_loads:
        copy.wait()

    wide_first = lax.broadcasted_iota(jnp.int32, (strip, lanes), 1) < rank_width

    def far(h, offset, c, read):
        base = jnp.bitwise_xor(me, offset) * pairs + c * chunk
        for u in range(chunk):
            ids = jnp.where(wide_first, cluster[2 * (base + u)], cluster[2 * (base + u) + 1])
            value = read(c * chunk + u)
            for w in range(targets):
                on = jnp.where(ids == w, 1.0, 0.0).astype(jnp.bfloat16)
                for c3 in range(components):
                    lhs[pl.ds(w * band + c3 * strip, strip), u * lanes : (u + 1) * lanes] = (
                        value[c3 * strip : (c3 + 1) * strip] * on
                    )
        basis = u_ref[pl.ds(base, chunk)].reshape(chunk * lanes, size)
        acc[h] += jnp.dot(lhs[...], basis, preferred_element_type=jnp.float32)

    def far_own(h):
        over_chunks(lambda c: far(h, 0, c, lambda m: sent[0, h, m]))

    def far_chunk(h, c):
        def one(offset):
            exchange(offset, h, c).wait_recv()
            far(h, offset, c, lambda m: got[offset - 1, h, m])

        over_offsets(one)

    portion = shards * kept * band

    def comp_copy(h, step):
        to = lax.rem(half_of + step, pairing)
        return pltpu.make_async_remote_copy(
            src_ref=acc.at[h, pl.ds(pl.multiple_of(to * portion, portion), portion)],
            dst_ref=comp_got.at[h, step - 1],
            send_sem=comp_send.at[h, step - 1],
            recv_sem=comp_recv.at[h, step - 1],
            device_id={"comp": to},
            device_id_type=MESH,
        )

    piece = kept * band

    def src_copy(h, step):
        to = lax.rem(row + step, shards)
        return pltpu.make_async_remote_copy(
            src_ref=cast.at[h, pl.ds(pl.multiple_of(to * piece, piece), piece)],
            dst_ref=src_got.at[h, step - 1],
            send_sem=src_send.at[h, step - 1],
            recv_sem=src_recv.at[h, step - 1],
            device_id={"src": to},
            device_id_type=MESH,
        )

    def share_comp(h):
        for step in range(1, pairing):
            comp_copy(h, step).start()

    def share_src(h):
        for step in range(1, pairing):
            comp_copy(h, step).wait_recv()
        value = acc[h, pl.ds(pl.multiple_of(half_of * portion, portion), portion), :]
        for step in range(1, pairing):
            value = value + comp_got[h, step - 1]
        total[h] = value
        cast[h] = value.astype(jnp.bfloat16)
        for step in range(1, shards):
            src_copy(h, step).start()

    def finish(h):
        value = total[h, pl.ds(pl.multiple_of(row * piece, piece), piece), :]
        for step in range(1, shards):
            src_copy(h, step).wait_recv()
            value = value + src_got[h, step - 1].astype(jnp.float32)
        for k in range(kept):
            for c in range(components):
                at = k * band + c * strip
                out_ref[c, h * strip : (h + 1) * strip, k * size : (k + 1) * size] = value[
                    at : at + strip
                ]

    for h in range(HALVES):
        far_own(h)
    for h in range(HALVES):
        over_chunks(functools.partial(far_chunk, h))
        share_comp(h)
        share_src(h)
        if h:
            finish(h - 1)
    finish(HALVES - 1)

    for h in range(HALVES):
        over_chunks(lambda c, h=h: over_offsets(lambda offset: exchange(offset, h, c).wait_send()))
        for step in range(1, pairing):
            comp_copy(h, step).wait_send()
        for step in range(1, shards):
            src_copy(h, step).wait_send()


def body(
    field,
    dest_group,
    src_local,
    ranks,
    mixing,
    v_factor,
    u_factor,
    slot_cluster,
    near_src,
    near_tgt,
    near_mixing,
    near_matrix,
):
    groups = lax.axis_size("tgt")
    shards = lax.axis_size("src")
    pairing = lax.axis_size("comp")
    blocks, rank_width, size = v_factor.shape
    components, vectors, points = field.shape
    channels = components * vectors
    owned = points // size
    slots = u_factor.shape[0]
    pairs = slots // groups // 2
    targets = owned * shards
    kept = targets // (pairing * shards)
    lanes = 2 * rank_width
    chunk = 8 if pairs % 8 == 0 else pairs
    chunks = pairs // chunk
    band = channels // HALVES
    near_count = near_matrix.shape[0]
    smem = pl.BlockSpec(memory_space=pltpu.SMEM)
    anywhere = pl.BlockSpec(memory_space=pl.ANY)
    f32, bf16, i32 = jnp.float32, jnp.bfloat16, jnp.int32
    dma = pltpu.SemaphoreType.DMA
    return pl.pallas_call(
        functools.partial(fused_kernel, (groups, shards, pairing, components, chunk)),
        out_shape=jax.ShapeDtypeStruct((components, vectors, kept * size), f32),
        in_specs=[anywhere] * 4 + [smem] + [anywhere] * 2 + [smem] * 4 + [anywhere],
        out_specs=pl.BlockSpec(memory_space=pltpu.VMEM),
        scratch_shapes=[
            pltpu.VMEM((channels, points), bf16),
            pltpu.VMEM((owned, channels, size), bf16),
            pltpu.VMEM((blocks, rank_width, size), bf16),
            pltpu.VMEM((slots // 2, lanes, size), bf16),
            pltpu.VMEM((near_count, size, size), bf16),
            pltpu.VMEM((3, 1, blocks), i32),
            pltpu.VMEM((8, slots), i32),
            pltpu.SMEM((8, slots), i32),
            pltpu.VMEM((HALVES, near_count, band, size), f32),
            pltpu.VMEM((groups, HALVES, pairs, band, lanes), bf16),
            pltpu.VMEM((groups - 1, HALVES, pairs, band, lanes), bf16),
            pltpu.VMEM((targets * band, chunk * lanes), bf16),
            pltpu.VMEM((HALVES, targets * band, size), f32),
            pltpu.VMEM((HALVES, pairing - 1, shards * kept * band, size), f32),
            pltpu.VMEM((HALVES, shards * kept * band, size), f32),
            pltpu.VMEM((HALVES, shards * kept * band, size), bf16),
            pltpu.VMEM((HALVES, shards - 1, kept * band, size), bf16),
            dma((9,)),
            dma((groups,)),
            dma,
            dma((HALVES, groups - 1, chunks)),
            dma((HALVES, groups - 1, chunks)),
            dma((HALVES, pairing - 1)),
            dma((HALVES, pairing - 1)),
            dma((HALVES, shards - 1)),
            dma((HALVES, shards - 1)),
        ],
        compiler_params=pltpu.CompilerParams(collective_id=0, has_side_effects=True),
        name="fused",
    )(
        field.reshape(channels, points),
        dest_group.reshape(1, -1),
        src_local.reshape(1, -1),
        ranks.reshape(1, -1),
        mixing.transpose(1, 2, 0),
        v_factor,
        u_factor.reshape(slots // 2, lanes, size),
        slot_cluster,
        near_src,
        near_tgt,
        near_mixing.transpose(1, 0, 2),
        near_matrix,
    )


def solution(mesh):
    everywhere = ("comp", "tgt", "src")
    placed = (
        P(None, None, ("tgt", "src")),
        P(everywhere, None),
        P(everywhere),
        P(everywhere),
        P(everywhere, None, None),
        P(everywhere, None, None),
        P(everywhere, None, None),
        P(everywhere),
        P(everywhere),
        P(everywhere),
        P(everywhere, None, None),
        P(everywhere, None, None),
    )
    return jax.shard_map(
        body,
        mesh=mesh,
        in_specs=placed,
        out_specs=P(None, None, everywhere),
        check_vma=False,
    )
```

```python
import functools
import math

import jax
import jax.numpy as jnp
from jax import lax
from jax.experimental import pallas as pl
from jax.experimental.pallas import tpu as pltpu
from jax.sharding import PartitionSpec as P

NT = (((1,), (1,)), ((), ()))
MESH = pl.DeviceIdType.MESH
HALVES = 2
TILE = 16
TILE_BITS = 4


def cut(length):
    plan, begin = [], 0
    while begin < length:
        left = length - begin
        size = 8 if left > 12 else min(left, max(4, left - 4))
        plan.append((begin, size))
        begin += size
    return tuple(plan)


def mix_rows(weights, parts):
    mixed = []
    for row in weights:
        total = row[0] * parts[0]
        for weight, part in zip(row[1:], parts[1:]):
            total = total + weight * part
        mixed.append(total)
    return mixed


def fused_kernel(
    sizes,
    field_hbm,
    dest_hbm,
    src_hbm,
    ranks_hbm,
    mix_hbm,
    v_hbm,
    u_hbm,
    cluster_hbm,
    near_src_hbm,
    near_tgt_hbm,
    near_mix_hbm,
    near_hbm,
    out_ref,
    field_ref,
    x_ref,
    v_ref,
    u_ref,
    near_ref,
    rows_ref,
    meta_ref,
    meta,
    mix_ref,
    cluster,
    near_src,
    near_tgt,
    near_mix,
    near_out,
    sent,
    got,
    lhs,
    acc,
    comp_got,
    total,
    cast,
    src_got,
    load_sem,
    u_sem,
    meta_sem,
    send_sem,
    recv_sem,
    comp_send,
    comp_recv,
    src_send,
    src_recv,
):
    groups, shards, pairing, components, chunk = sizes
    me = lax.axis_index("tgt")
    row = lax.axis_index("src")
    half_of = lax.axis_index("comp")
    owned, channels, size = x_ref.shape
    vectors = channels // components
    strip = vectors // HALVES
    band = components * strip
    slots, rank_width = u_hbm.shape[0] * 2, u_hbm.shape[1] // 2
    blocks = v_hbm.shape[0]
    capacity = slots // groups
    pairs = capacity // 2
    lanes = 2 * rank_width
    chunks = pairs // chunk
    targets = acc.shape[1] // band
    kept = targets // (pairing * shards)

    def load(index, source, target):
        return pltpu.make_async_copy(source, target, load_sem.at[index])

    small = [
        load(0, dest_hbm, rows_ref.at[0]),
        load(1, ranks_hbm, rows_ref.at[1]),
        load(2, src_hbm, rows_ref.at[2]),
    ]
    early = [load(3, field_hbm, field_ref), load(4, mix_hbm, mix_ref)]
    later = [
        load(9, near_hbm, near_ref),
        load(10, cluster_hbm, cluster),
        load(11, near_src_hbm, near_src),
        load(12, near_tgt_hbm, near_tgt),
        load(13, near_mix_hbm, near_mix),
    ]
    split = 4 if blocks % 4 == 0 else 1
    part = blocks // split
    v_loads = [
        load(5 + i, v_hbm.at[pl.ds(i * part, part)], v_ref.at[pl.ds(i * part, part)])
        for i in range(split)
    ]
    u_loads = [
        pltpu.make_async_copy(
            u_hbm.at[pl.ds(g * pairs, pairs)], u_ref.at[pl.ds(g * pairs, pairs)], u_sem.at[g]
        )
        for g in range(groups)
    ]
    for copy in small + early + v_loads:
        copy.start()

    barrier = pltpu.get_barrier_semaphore()
    for step in range(1, groups):
        pl.semaphore_signal(
            barrier, inc=1, device_id={"tgt": jnp.bitwise_xor(me, step)}, device_id_type=MESH
        )
    for step in range(1, shards):
        pl.semaphore_signal(
            barrier, inc=1, device_id={"src": lax.rem(row + step, shards)}, device_id_type=MESH
        )
    for step in range(1, pairing):
        pl.semaphore_signal(
            barrier, inc=1, device_id={"comp": lax.rem(half_of + step, pairing)}, device_id_type=MESH
        )

    for copy in small:
        copy.wait()
    dest = rows_ref[0]
    padded = -(-groups // 16) * 16
    member = jnp.where(
        lax.broadcasted_iota(jnp.int32, (padded, blocks), 0) == dest, 1.0, 0.0
    )
    before = jnp.where(
        lax.broadcasted_iota(jnp.int32, (blocks, blocks), 0)
        < lax.broadcasted_iota(jnp.int32, (blocks, blocks), 1),
        1.0,
        0.0,
    ).astype(jnp.bfloat16)
    earlier = jnp.dot(member.astype(jnp.bfloat16), before, preferred_element_type=jnp.float32)
    position = jnp.sum(member * earlier, axis=0, keepdims=True)
    slot = dest * capacity + position.astype(jnp.int32)
    taken = jnp.where(
        lax.broadcasted_iota(jnp.int32, (slots, blocks), 0) == slot, 1.0, 0.0
    ).astype(jnp.bfloat16)
    line = lax.broadcasted_iota(jnp.int32, (16, blocks), 0)
    facts = jnp.where(
        line == 0,
        lax.broadcasted_iota(jnp.int32, (16, blocks), 1),
        jnp.where(line == 1, rows_ref[1], rows_ref[2]),
    )
    placed = lax.dot_general(
        facts.astype(jnp.float32).astype(jnp.bfloat16), taken, NT, preferred_element_type=jnp.float32
    )
    meta_ref[...] = placed[:8].astype(jnp.int32)
    to_scalars = pltpu.make_async_copy(meta_ref, meta, meta_sem)
    to_scalars.start()

    early[0].wait()
    for s in range(owned):
        x_ref[s] = field_ref[:, s * size : (s + 1) * size]
    to_scalars.wait()
    for copy in early[1:] + v_loads:
        copy.wait()
    for copy in later + u_loads:
        copy.start()

    lane = lax.broadcasted_iota(jnp.int32, (1, lanes), 1)
    first = lane < rank_width
    rank_at = lane % rank_width
    unroll = 4 if chunk % 4 == 0 else 1

    def coef_step(offset, start):
        base = jnp.bitwise_xor(me, offset) * capacity + 2 * start
        numbers = [jnp.clip(meta[0, base + i], 0, blocks - 1) for i in range(2 * unroll)]
        v = jnp.concatenate([v_ref[b] for b in numbers], axis=0)
        x = x_ref[...].reshape(owned * channels, size)
        y = lax.dot_general(x, v, NT, preferred_element_type=jnp.float32)
        for u in range(unroll):
            b0, b1 = numbers[2 * u], numbers[2 * u + 1]
            k0, k1 = base + 2 * u, base + 2 * u + 1
            here = y[:, u * lanes : (u + 1) * lanes]
            chosen = jnp.where(first, meta[2, k0], meta[2, k1])
            coef = here[:channels]
            for s in range(1, owned):
                coef = jnp.where(chosen == s, here[s * channels : (s + 1) * channels], coef)
            coef = jnp.where(rank_at < jnp.where(first, meta[1, k0], meta[1, k1]), coef, 0.0)
            weights = [
                [jnp.where(first, mix_ref[c, d, b0], mix_ref[c, d, b1]) for d in range(components)]
                for c in range(components)
            ]
            mixed = mix_rows(
                weights, [coef[d * vectors : (d + 1) * vectors] for d in range(components)]
            )
            for h in range(HALVES):
                for c in range(components):
                    sent[offset, h, start + u, c * strip : (c + 1) * strip, :] = mixed[c][
                        h * strip : (h + 1) * strip
                    ].astype(jnp.bfloat16)

    def coef_chunk(offset, c):
        def several(step, carry):
            coef_step(offset, c * chunk + step * unroll)
            return carry

        lax.fori_loop(0, chunk // unroll, several, 0)

    def exchange(offset, h, c):
        where = (h, pl.ds(c * chunk, chunk))
        return pltpu.make_async_remote_copy(
            src_ref=sent.at[(offset,) + where],
            dst_ref=got.at[(offset - 1,) + where],
            send_sem=send_sem.at[h, offset - 1, c],
            recv_sem=recv_sem.at[h, offset - 1, c],
            device_id={"tgt": jnp.bitwise_xor(me, offset)},
            device_id_type=MESH,
        )

    def over_offsets(action):
        def step(t, carry):
            action(groups - 1 - t)
            return carry

        lax.fori_loop(0, groups - 1, step, 0)

    def over_chunks(action):
        def step(c, carry):
            action(c)
            return carry

        lax.fori_loop(0, chunks, step, 0)

    pl.semaphore_wait(barrier, groups + shards + pairing - 3)

    def send_first(c):
        def one(offset):
            coef_chunk(offset, c)
            exchange(offset, 0, c).start()

        over_offsets(one)

    over_chunks(send_first)
    for h in range(1, HALVES):
        over_chunks(lambda c, h=h: over_offsets(lambda offset: exchange(offset, h, c).start()))
    over_chunks(lambda c: coef_chunk(0, c))

    for copy in later:
        copy.wait()
    for n in range(near_ref.shape[0]):
        y = lax.dot_general(
            x_ref[near_src[n]], near_ref[n], NT, preferred_element_type=jnp.float32
        )
        weights = [[near_mix[c, n, d] for d in range(components)] for c in range(components)]
        mixed = mix_rows(weights, [y[d * vectors : (d + 1) * vectors] for d in range(components)])
        for h in range(HALVES):
            for c in range(components):
                near_out[h, n, c * strip : (c + 1) * strip, :] = mixed[c][
                    h * strip : (h + 1) * strip
                ]

    def place_near(w, carry):
        for h in range(HALVES):
            value = jnp.where(near_tgt[0] == w, near_out[h, 0], 0.0)
            for n in range(1, near_ref.shape[0]):
                value = value + jnp.where(near_tgt[n] == w, near_out[h, n], 0.0)
            acc[h, pl.ds(pl.multiple_of(w * band, band), band), :] = value
        return carry

    lax.fori_loop(0, targets, place_near, 0)
    for copy in u_loads:
        copy.wait()

    wide_first = lax.broadcasted_iota(jnp.int32, (strip, lanes), 1) < rank_width

    def far(h, offset, c, read):
        base = jnp.bitwise_xor(me, offset) * pairs + c * chunk
        for u in range(chunk):
            ids = jnp.where(wide_first, cluster[2 * (base + u)], cluster[2 * (base + u) + 1])
            value = read(c * chunk + u)
            for w in range(targets):
                on = jnp.where(ids == w, 1.0, 0.0).astype(jnp.bfloat16)
                for c3 in range(components):
                    lhs[pl.ds(w * band + c3 * strip, strip), u * lanes : (u + 1) * lanes] = (
                        value[c3 * strip : (c3 + 1) * strip] * on
                    )
        basis = u_ref[pl.ds(base, chunk)].reshape(chunk * lanes, size)
        acc[h] += jnp.dot(lhs[...], basis, preferred_element_type=jnp.float32)

    def far_own(h):
        over_chunks(lambda c: far(h, 0, c, lambda m: sent[0, h, m]))

    def far_chunk(h, c):
        def one(offset):
            exchange(offset, h, c).wait_recv()
            far(h, offset, c, lambda m: got[offset - 1, h, m])

        over_offsets(one)

    portion = shards * kept * band

    def comp_copy(h, step):
        to = lax.rem(half_of + step, pairing)
        return pltpu.make_async_remote_copy(
            src_ref=acc.at[h, pl.ds(pl.multiple_of(to * portion, portion), portion)],
            dst_ref=comp_got.at[h, step - 1],
            send_sem=comp_send.at[h, step - 1],
            recv_sem=comp_recv.at[h, step - 1],
            device_id={"comp": to},
            device_id_type=MESH,
        )

    piece = kept * band

    def src_copy(h, step):
        to = lax.rem(row + step, shards)
        return pltpu.make_async_remote_copy(
            src_ref=cast.at[h, pl.ds(pl.multiple_of(to * piece, piece), piece)],
            dst_ref=src_got.at[h, step - 1],
            send_sem=src_send.at[h, step - 1],
            recv_sem=src_recv.at[h, step - 1],
            device_id={"src": to},
            device_id_type=MESH,
        )

    def share_comp(h):
        for step in range(1, pairing):
            comp_copy(h, step).start()

    def share_src(h):
        for step in range(1, pairing):
            comp_copy(h, step).wait_recv()
        value = acc[h, pl.ds(pl.multiple_of(half_of * portion, portion), portion), :]
        for step in range(1, pairing):
            value = value + comp_got[h, step - 1]
        total[h] = value
        cast[h] = value.astype(jnp.bfloat16)
        for step in range(1, shards):
            src_copy(h, step).start()

    def finish(h):
        value = total[h, pl.ds(pl.multiple_of(row * piece, piece), piece), :]
        for step in range(1, shards):
            src_copy(h, step).wait_recv()
            value = value + src_got[h, step - 1].astype(jnp.float32)
        for k in range(kept):
            for c in range(components):
                at = k * band + c * strip
                out_ref[c, h * strip : (h + 1) * strip, k * size : (k + 1) * size] = value[
                    at : at + strip
                ]

    for h in range(HALVES):
        far_own(h)
    for h in range(HALVES):
        over_chunks(functools.partial(far_chunk, h))
        share_comp(h)
        share_src(h)
        if h:
            finish(h - 1)
    finish(HALVES - 1)

    for h in range(HALVES):
        over_chunks(lambda c, h=h: over_offsets(lambda offset: exchange(offset, h, c).wait_send()))
        for step in range(1, pairing):
            comp_copy(h, step).wait_send()
        for step in range(1, shards):
            src_copy(h, step).wait_send()


def packed_kernel(
    sizes,
    field_hbm,
    dest_hbm,
    src_hbm,
    ranks_hbm,
    mix_hbm,
    v_hbm,
    u_hbm,
    cluster_hbm,
    near_src_hbm,
    near_tgt_hbm,
    near_mix_hbm,
    near_hbm,
    out_ref,
    flag_ref,
    field_ref,
    x_ref,
    v_ref,
    u_ref,
    near_ref,
    rows_ref,
    meta_ref,
    meta,
    mix_ref,
    weight_ref,
    table_got,
    table,
    flag_row,
    flag_got,
    cluster,
    near_src,
    near_tgt,
    near_mix,
    near_out,
    sent,
    got,
    lhs,
    rhs,
    acc,
    comp_got,
    total,
    cast,
    src_got,
    load_sem,
    u_sem,
    meta_sem,
    send_sem,
    recv_sem,
    comp_send,
    comp_recv,
    src_send,
    src_recv,
    table_send,
    table_recv,
    table_sem,
    flag_send,
    flag_recv,
):
    groups, shards, pairing, components, limit, plan = sizes
    me = lax.axis_index("tgt")
    row = lax.axis_index("src")
    half_of = lax.axis_index("comp")
    owned, channels, size = x_ref.shape
    vectors = channels // components
    strip = vectors // HALVES
    band = components * strip
    lanes = sent.shape[-1]
    tiles_in = lanes // TILE
    whole = sent.shape[2]
    full = whole * tiles_in
    blocks = weight_ref.shape[0]
    tiles = v_hbm.shape[0]
    per_block = tiles // blocks
    capacity = full // per_block
    targets = acc.shape[1] // band
    kept = targets // (pairing * shards)

    def load(index, source, target):
        return pltpu.make_async_copy(source, target, load_sem.at[index])

    small = [
        load(0, dest_hbm, rows_ref.at[0]),
        load(1, ranks_hbm, rows_ref.at[1]),
        load(2, src_hbm, rows_ref.at[2]),
    ]
    early = [load(3, field_hbm, field_ref), load(4, mix_hbm, mix_ref)]
    later = [
        load(9, near_hbm, near_ref),
        load(10, cluster_hbm, cluster),
        load(11, near_src_hbm, near_src),
        load(12, near_tgt_hbm, near_tgt),
        load(13, near_mix_hbm, near_mix),
    ]
    split = 4 if tiles % 4 == 0 else 1
    part = tiles // split
    v_loads = [
        load(5 + i, v_hbm.at[pl.ds(i * part, part)], v_ref.at[pl.ds(i * part, part)])
        for i in range(split)
    ]
    u_loads = [
        pltpu.make_async_copy(
            u_hbm.at[pl.ds(g * full, full)], u_ref.at[pl.ds(g * full, full)], u_sem.at[g]
        )
        for g in range(groups)
    ]
    for copy in small + early + v_loads:
        copy.start()

    barrier = pltpu.get_barrier_semaphore()
    for step in range(1, groups):
        pl.semaphore_signal(
            barrier, inc=1, device_id={"tgt": jnp.bitwise_xor(me, step)}, device_id_type=MESH
        )
    for step in range(1, shards):
        pl.semaphore_signal(
            barrier, inc=1, device_id={"src": lax.rem(row + step, shards)}, device_id_type=MESH
        )
    for step in range(1, pairing):
        pl.semaphore_signal(
            barrier, inc=1, device_id={"comp": lax.rem(half_of + step, pairing)}, device_id_type=MESH
        )

    for copy in small:
        copy.wait()
    dest, rank, source = rows_ref[0], rows_ref[1], rows_ref[2]
    count = lax.shift_right_logical(rank + (TILE - 1), TILE_BITS)
    padded = -(-groups // 16) * 16
    group_at = lax.broadcasted_iota(jnp.int32, (padded, blocks), 0)
    member = jnp.where(group_at == dest, 1.0, 0.0)
    both = jnp.concatenate([member, member * count.astype(jnp.float32)], axis=0)
    before = jnp.where(
        lax.broadcasted_iota(jnp.int32, (blocks, blocks), 0)
        < lax.broadcasted_iota(jnp.int32, (blocks, blocks), 1),
        1.0,
        0.0,
    ).astype(jnp.bfloat16)
    earlier = jnp.dot(both.astype(jnp.bfloat16), before, preferred_element_type=jnp.float32)
    position = jnp.sum(member * earlier[:padded], axis=0, keepdims=True).astype(jnp.int32)
    tile_at = jnp.sum(member * earlier[padded:], axis=0, keepdims=True).astype(jnp.int32)
    used = jnp.sum(both[padded:], axis=1, keepdims=True)
    away = lax.broadcasted_iota(jnp.int32, (padded, 1), 0) != me
    most = jnp.max(jnp.where(away, used, 0.0), axis=0, keepdims=True)
    over = jnp.where(most > float(limit * tiles_in), 1, 0)
    start = dest * full + tile_at
    ahead = lax.broadcasted_iota(jnp.int32, (groups * full, blocks), 0) - start
    taken = jnp.where((ahead >= 0) & (ahead < count), 1.0, 0.0).astype(jnp.bfloat16)
    line = lax.broadcasted_iota(jnp.int32, (16, blocks), 0)
    facts = jnp.where(line == 0, lax.broadcasted_iota(jnp.int32, (16, blocks), 1), 1)
    for at, fact in enumerate((rank, source, position, tile_at)):
        facts = jnp.where(line == at + 1, fact, facts)
    placed = lax.dot_general(
        facts.astype(jnp.float32).astype(jnp.bfloat16), taken, NT, preferred_element_type=jnp.float32
    )
    placed = placed.astype(jnp.int32)
    where_at = lax.broadcasted_iota(jnp.int32, (1, groups * full), 1) % full
    sub = jnp.where(placed[5:6] > 0, where_at - placed[4:5], 0)
    table_rows = [
        placed[0:1] * per_block + sub,
        placed[0:1],
        placed[2:3],
        jnp.clip(placed[1:2] - TILE * sub, 0, TILE),
        placed[3:4] * per_block + sub,
        jnp.broadcast_to(over, (1, groups * full)),
    ]
    table_rows = jnp.concatenate(table_rows + table_rows[-1:] * 2, axis=0)
    for g in range(groups):
        meta_ref[g] = table_rows[:, g * full : (g + 1) * full]
    to_scalars = pltpu.make_async_copy(meta_ref, meta, meta_sem)
    to_scalars.start()

    early[1].wait()
    entries = [mix_ref[c, d : d + 1, :] for c in range(components) for d in range(components)]
    entries = jnp.concatenate(entries + entries[:1] * (16 - len(entries)), axis=0)
    for b in range(blocks):
        weight_ref[b] = jnp.broadcast_to(entries[:, b : b + 1], (16, lanes))

    early[0].wait()
    for s in range(owned):
        x_ref[s] = field_ref[:, s * size : (s + 1) * size]
    to_scalars.wait()
    for copy in v_loads:
        copy.wait()
    for copy in later + u_loads:
        copy.start()

    lane = lax.broadcasted_iota(jnp.int32, (1, lanes), 1)
    in_tile = lane % TILE
    tile_of = lane // TILE

    def spread(values):
        vector = values[0]
        for i, value in enumerate(values[1:]):
            vector = jnp.where(tile_of == i + 1, value, vector)
        return vector

    def coef_step(offset, start, unroll):
        to = jnp.bitwise_xor(me, offset)

        def entry(fact, u, i):
            return meta[to, fact, (start + u) * tiles_in + i]

        v = jnp.concatenate(
            [
                v_ref[jnp.clip(entry(0, u, i), 0, tiles - 1)]
                for u in range(unroll)
                for i in range(tiles_in)
            ],
            axis=0,
        )
        x = x_ref[...].reshape(owned * channels, size)
        y = lax.dot_general(x, v, NT, preferred_element_type=jnp.float32)
        for u in range(unroll):
            here = y[:, u * lanes : (u + 1) * lanes]
            chosen = spread([entry(2, u, i) for i in range(tiles_in)])
            coef = here[:channels]
            for s in range(1, owned):
                coef = jnp.where(chosen == s, here[s * channels : (s + 1) * channels], coef)
            coef = jnp.where(in_tile < spread([entry(3, u, i) for i in range(tiles_in)]), coef, 0.0)
            weight = spread(
                [weight_ref[jnp.clip(entry(1, u, i), 0, blocks - 1)] for i in range(tiles_in)]
            )
            weights = [
                [weight[c * components + d : c * components + d + 1] for d in range(components)]
                for c in range(components)
            ]
            mixed = mix_rows(
                weights, [coef[d * vectors : (d + 1) * vectors] for d in range(components)]
            )
            for h in range(HALVES):
                for c in range(components):
                    sent[offset, h, start + u, c * strip : (c + 1) * strip, :] = mixed[c][
                        h * strip : (h + 1) * strip
                    ].astype(jnp.bfloat16)

    def coef_chunk(offset, begin, length):
        unroll = next(u for u in (4, 3, 2, 1) if length % u == 0)

        def several(step, carry):
            coef_step(offset, begin + step * unroll, unroll)
            return carry

        lax.fori_loop(0, length // unroll, several, 0)

    def exchange(offset, h, c):
        where = (h, pl.ds(*plan[c]))
        return pltpu.make_async_remote_copy(
            src_ref=sent.at[(offset,) + where],
            dst_ref=got.at[(offset - 1,) + where],
            send_sem=send_sem.at[h, offset - 1, c],
            recv_sem=recv_sem.at[h, offset - 1, c],
            device_id={"tgt": jnp.bitwise_xor(me, offset)},
            device_id_type=MESH,
        )

    def over_offsets(action):
        def step(t, carry):
            action(groups - 1 - t)
            return carry

        lax.fori_loop(0, groups - 1, step, 0)

    def table_copy(offset):
        to = jnp.bitwise_xor(me, offset)
        return pltpu.make_async_remote_copy(
            src_ref=meta_ref.at[to],
            dst_ref=table_got.at[offset - 1],
            send_sem=table_send.at[offset - 1],
            recv_sem=table_recv.at[offset - 1],
            device_id={"tgt": to},
            device_id_type=MESH,
        )

    def table_down(offset):
        return pltpu.make_async_copy(
            table_got.at[offset - 1], table.at[offset - 1], table_sem.at[offset - 1]
        )

    pl.semaphore_wait(barrier, groups + shards + pairing - 3)
    over_offsets(lambda offset: table_copy(offset).start())
    for c, (begin, length) in enumerate(plan):

        def one(offset):
            coef_chunk(offset, begin, length)
            exchange(offset, 0, c).start()

        over_offsets(one)
    for h in range(1, HALVES):
        for c in range(len(plan)):
            over_offsets(lambda offset: exchange(offset, h, c).start())
    coef_chunk(0, 0, whole)

    def fetch(offset):
        table_copy(offset).wait_recv()
        table_down(offset).start()

    over_offsets(fetch)
    for copy in later:
        copy.wait()
    for n in range(near_ref.shape[0]):
        y = lax.dot_general(
            x_ref[near_src[n]], near_ref[n], NT, preferred_element_type=jnp.float32
        )
        weights = [[near_mix[c, n, d] for d in range(components)] for c in range(components)]
        mixed = mix_rows(weights, [y[d * vectors : (d + 1) * vectors] for d in range(components)])
        for h in range(HALVES):
            for c in range(components):
                near_out[h, n, c * strip : (c + 1) * strip, :] = mixed[c][
                    h * strip : (h + 1) * strip
                ]

    def place_near(w, carry):
        for h in range(HALVES):
            value = jnp.where(near_tgt[0] == w, near_out[h, 0], 0.0)
            for n in range(1, near_ref.shape[0]):
                value = value + jnp.where(near_tgt[n] == w, near_out[h, n], 0.0)
            acc[h, pl.ds(pl.multiple_of(w * band, band), band), :] = value
        return carry

    lax.fori_loop(0, targets, place_near, 0)
    for copy in u_loads:
        copy.wait()

    wide_tile = lax.broadcasted_iota(jnp.int32, (strip, lanes), 1) // TILE

    def far(h, sender, entry, begin, length, read):
        for u in range(length):
            ids = None
            for i in range(tiles_in):
                at = jnp.clip(entry((begin + u) * tiles_in + i), 0, full - 1)
                rhs[u * lanes + i * TILE : u * lanes + (i + 1) * TILE, :] = u_ref[sender * full + at]
                target = cluster[sender * capacity + lax.div(at, per_block)]
                ids = jnp.full((strip, lanes), target) if i == 0 else jnp.where(wide_tile == i, target, ids)
            value = read(begin + u)
            for w in range(targets):
                on = jnp.where(ids == w, 1.0, 0.0).astype(jnp.bfloat16)
                for c3 in range(components):
                    lhs[pl.ds(w * band + c3 * strip, strip), u * lanes : (u + 1) * lanes] = (
                        value[c3 * strip : (c3 + 1) * strip] * on
                    )
        acc[h] += jnp.dot(
            lhs[:, : length * lanes], rhs[: length * lanes], preferred_element_type=jnp.float32
        )

    def far_own(h):
        block = 8 if whole % 8 == 0 else 1

        def several(c, carry):
            far(h, me, lambda t: meta[me, 4, t], c * block, block, lambda m: sent[0, h, m])
            return carry

        lax.fori_loop(0, whole // block, several, 0)

    def far_chunk(h, c):
        def one(offset):
            exchange(offset, h, c).wait_recv()
            far(
                h,
                jnp.bitwise_xor(me, offset),
                lambda t: table[offset - 1, 4, t],
                *plan[c],
                lambda m: got[offset - 1, h, m],
            )

        over_offsets(one)

    def flag_copy(step):
        axis, place, span, by = (
            ("comp", half_of, pairing, step) if step < pairing else ("src", row, shards, step - pairing + 1)
        )
        kind = 0 if axis == "comp" else 1
        return pltpu.make_async_remote_copy(
            src_ref=flag_row.at[kind],
            dst_ref=flag_got.at[step - 1],
            send_sem=flag_send.at[step - 1],
            recv_sem=flag_recv.at[step - 1],
            device_id={axis: lax.rem(place + by, span)},
            device_id_type=MESH,
        )

    comp_steps = range(1, pairing)
    src_steps = range(pairing, pairing + shards - 1)

    portion = shards * kept * band

    def comp_copy(h, step):
        to = lax.rem(half_of + step, pairing)
        return pltpu.make_async_remote_copy(
            src_ref=acc.at[h, pl.ds(pl.multiple_of(to * portion, portion), portion)],
            dst_ref=comp_got.at[h, step - 1],
            send_sem=comp_send.at[h, step - 1],
            recv_sem=comp_recv.at[h, step - 1],
            device_id={"comp": to},
            device_id_type=MESH,
        )

    piece = kept * band

    def src_copy(h, step):
        to = lax.rem(row + step, shards)
        return pltpu.make_async_remote_copy(
            src_ref=cast.at[h, pl.ds(pl.multiple_of(to * piece, piece), piece)],
            dst_ref=src_got.at[h, step - 1],
            send_sem=src_send.at[h, step - 1],
            recv_sem=src_recv.at[h, step - 1],
            device_id={"src": to},
            device_id_type=MESH,
        )

    def share_comp(h):
        for step in range(1, pairing):
            comp_copy(h, step).start()

    def share_src(h):
        for step in range(1, pairing):
            comp_copy(h, step).wait_recv()
        value = acc[h, pl.ds(pl.multiple_of(half_of * portion, portion), portion), :]
        for step in range(1, pairing):
            value = value + comp_got[h, step - 1]
        total[h] = value
        cast[h] = value.astype(jnp.bfloat16)
        for step in range(1, shards):
            src_copy(h, step).start()

    def finish(h):
        value = total[h, pl.ds(pl.multiple_of(row * piece, piece), piece), :]
        for step in range(1, shards):
            src_copy(h, step).wait_recv()
            value = value + src_got[h, step - 1].astype(jnp.float32)
        for k in range(kept):
            for c in range(components):
                at = k * band + c * strip
                out_ref[c, h * strip : (h + 1) * strip, k * size : (k + 1) * size] = value[
                    at : at + strip
                ]

    seen = over
    for offset in range(1, groups):
        seen = jnp.maximum(seen, table_got[offset - 1, 5:6, 0:1])
        table_down(offset).wait()
    flag_row[0] = jnp.broadcast_to(seen, flag_row.shape[1:])
    for step in comp_steps:
        flag_copy(step).start()
    far_own(0)
    seen = flag_row[0]
    for step in comp_steps:
        flag_copy(step).wait_recv()
        seen = jnp.maximum(seen, flag_got[step - 1])
    flag_row[1] = seen
    for step in src_steps:
        flag_copy(step).start()
    for h in range(1, HALVES):
        far_own(h)
    seen = flag_row[1]
    for step in src_steps:
        flag_copy(step).wait_recv()
        seen = jnp.maximum(seen, flag_got[step - 1])
    flag_ref[...] = seen
    for h in range(HALVES):
        for c in range(len(plan)):
            far_chunk(h, c)
        share_comp(h)
        share_src(h)
        if h:
            finish(h - 1)
    finish(HALVES - 1)

    over_offsets(lambda offset: table_copy(offset).wait_send())
    for step in list(comp_steps) + list(src_steps):
        flag_copy(step).wait_send()
    for h in range(HALVES):
        for c in range(len(plan)):
            over_offsets(lambda offset: exchange(offset, h, c).wait_send())
        for step in range(1, pairing):
            comp_copy(h, step).wait_send()
        for step in range(1, shards):
            src_copy(h, step).wait_send()


def body(
    field,
    dest_group,
    src_local,
    ranks,
    mixing,
    v_factor,
    u_factor,
    slot_cluster,
    near_src,
    near_tgt,
    near_mixing,
    near_matrix,
):
    groups = lax.axis_size("tgt")
    shards = lax.axis_size("src")
    pairing = lax.axis_size("comp")
    blocks, rank_width, size = v_factor.shape
    components, vectors, points = field.shape
    channels = components * vectors
    owned = points // size
    slots = u_factor.shape[0]
    pairs = slots // groups // 2
    targets = owned * shards
    kept = targets // (pairing * shards)
    lanes = 2 * rank_width
    band = channels // HALVES
    near_count = near_matrix.shape[0]
    portion = shards * kept * band
    f32, bf16, i32 = jnp.float32, jnp.bfloat16, jnp.int32
    dma = pltpu.SemaphoreType.DMA
    result = pltpu.VMEM((components, vectors, kept * size), f32)
    inputs = (
        field.reshape(channels, points),
        dest_group.reshape(1, -1),
        src_local.reshape(1, -1),
        ranks.reshape(1, -1),
        mixing.transpose(1, 2, 0),
    )
    near_inputs = (
        slot_cluster,
        near_src,
        near_tgt,
        near_mixing.transpose(1, 0, 2),
        near_matrix,
    )
    near_scalars = [
        pltpu.SMEM((slots,), i32),
        pltpu.SMEM((near_count,), i32),
        pltpu.SMEM((near_count,), i32),
        pltpu.SMEM((components, near_count, components), f32),
        pltpu.VMEM((HALVES, near_count, band, size), f32),
    ]
    reduce_buffers = [
        pltpu.VMEM((HALVES, targets * band, size), f32),
        pltpu.VMEM((HALVES, pairing - 1, portion, size), f32),
        pltpu.VMEM((HALVES, portion, size), f32),
        pltpu.VMEM((HALVES, portion, size), bf16),
        pltpu.VMEM((HALVES, shards - 1, kept * band, size), bf16),
        dma((14,)),
        dma((groups,)),
        dma,
    ]
    reduce_sems = [
        dma((HALVES, pairing - 1)),
        dma((HALVES, pairing - 1)),
        dma((HALVES, shards - 1)),
        dma((HALVES, shards - 1)),
    ]
    field_buffers = [
        pltpu.VMEM((channels, points), bf16),
        pltpu.VMEM((owned, channels, size), bf16),
    ]

    def padded():
        chunk = 8 if pairs % 8 == 0 else pairs
        return pl.pallas_call(
            functools.partial(fused_kernel, (groups, shards, pairing, components, chunk)),
            out_shape=result,
            in_specs=[pl.BlockSpec(memory_space=pl.ANY)] * 12,
            out_specs=pl.BlockSpec(memory_space=pltpu.VMEM),
            scratch_shapes=field_buffers
            + [
                pltpu.VMEM((blocks, rank_width, size), bf16),
                pltpu.VMEM((slots // 2, lanes, size), bf16),
                pltpu.VMEM((near_count, size, size), bf16),
                pltpu.VMEM((3, 1, blocks), i32),
                pltpu.VMEM((8, slots), i32),
                pltpu.SMEM((8, slots), i32),
                pltpu.SMEM((components, components, blocks), f32),
            ]
            + near_scalars
            + [
                pltpu.VMEM((groups, HALVES, pairs, band, lanes), bf16),
                pltpu.VMEM((groups - 1, HALVES, pairs, band, lanes), bf16),
                pltpu.VMEM((targets * band, chunk * lanes), bf16),
            ]
            + reduce_buffers
            + [dma((HALVES, groups - 1, pairs // chunk))] * 2
            + reduce_sems,
            compiler_params=pltpu.CompilerParams(collective_id=1, has_side_effects=True),
            name="padded",
        )(*inputs, v_factor, u_factor.reshape(slots // 2, lanes, size), *near_inputs)

    per_block = rank_width // TILE
    tiles_in = lanes // TILE
    full = slots // groups * per_block
    whole = full // tiles_in
    share = 0.68 + (slots // groups) ** -0.5
    limit = min(whole, math.ceil(whole * share))
    plan = cut(limit)
    value, flag = pl.pallas_call(
        functools.partial(packed_kernel, (groups, shards, pairing, components, limit, plan)),
        out_shape=(result, pltpu.VMEM((8, lanes), i32)),
        in_specs=[pl.BlockSpec(memory_space=pl.ANY)] * 12,
        out_specs=(pl.BlockSpec(memory_space=pltpu.VMEM),) * 2,
        scratch_shapes=field_buffers
        + [
            pltpu.VMEM((blocks * per_block, TILE, size), bf16),
            pltpu.VMEM((slots * per_block, TILE, size), bf16),
            pltpu.VMEM((near_count, size, size), bf16),
            pltpu.VMEM((3, 1, blocks), i32),
            pltpu.VMEM((groups, 8, full), i32),
            pltpu.SMEM((groups, 8, full), i32),
            pltpu.VMEM((components, components, blocks), f32),
            pltpu.VMEM((blocks, 16, lanes), f32),
            pltpu.VMEM((groups - 1, 8, full), i32),
            pltpu.SMEM((groups - 1, 8, full), i32),
            pltpu.VMEM((2, 8, lanes), i32),
            pltpu.VMEM((pairing + shards - 2, 8, lanes), i32),
        ]
        + near_scalars
        + [
            pltpu.VMEM((groups, HALVES, whole, band, lanes), bf16),
            pltpu.VMEM((groups - 1, HALVES, limit, band, lanes), bf16),
            pltpu.VMEM((targets * band, 8 * lanes), bf16),
            pltpu.VMEM((8 * lanes, size), bf16),
        ]
        + reduce_buffers
        + [dma((HALVES, groups - 1, len(plan)))] * 2
        + reduce_sems
        + [dma((groups - 1,))] * 3
        + [dma((pairing + shards - 2,))] * 2,
        compiler_params=pltpu.CompilerParams(collective_id=0, has_side_effects=True),
        name="packed",
    )(
        *inputs,
        v_factor.reshape(blocks * per_block, TILE, size),
        u_factor.reshape(slots * per_block, TILE, size),
        *near_inputs,
    )
    if limit == whole:
        return value
    return lax.cond(flag[0, 0] > 0, padded, lambda: value)


def solution(mesh):
    everywhere = ("comp", "tgt", "src")
    placed = (
        P(None, None, ("tgt", "src")),
        P(everywhere, None),
        P(everywhere),
        P(everywhere),
        P(everywhere, None, None),
        P(everywhere, None, None),
        P(everywhere, None, None),
        P(everywhere),
        P(everywhere),
        P(everywhere),
        P(everywhere, None, None),
        P(everywhere, None, None),
    )
    return jax.shard_map(
        body,
        mesh=mesh,
        in_specs=placed,
        out_specs=P(None, None, everywhere),
        check_vma=False,
    )
```

```python
import functools
import math

import jax
import jax.numpy as jnp
from jax import lax
from jax.experimental import pallas as pl
from jax.experimental.pallas import tpu as pltpu
from jax.sharding import PartitionSpec as P

NT = (((1,), (1,)), ((), ()))
MESH = pl.DeviceIdType.MESH
HALVES = 2
TILE = 16
TILE_BITS = 4


def cut(length):
    if length <= 8:
        return ((0, length),)
    plan, begin = [], 0
    while length - begin > 9:
        plan.append((begin, 8))
        begin += 8
    most = (2 * (length - begin) + 2) // 3
    plan.append((begin, most))
    if length - begin > most:
        plan.append((begin + most, length - begin - most))
    return tuple(plan)


def mix_rows(weights, parts):
    mixed = []
    for row in weights:
        total = row[0] * parts[0]
        for weight, part in zip(row[1:], parts[1:]):
            total = total + weight * part
        mixed.append(total)
    return mixed


def fused_kernel(
    sizes,
    field_hbm,
    dest_hbm,
    src_hbm,
    ranks_hbm,
    mix_hbm,
    v_hbm,
    u_hbm,
    cluster_hbm,
    near_src_hbm,
    near_tgt_hbm,
    near_mix_hbm,
    near_hbm,
    out_ref,
    field_ref,
    x_ref,
    v_ref,
    u_ref,
    near_ref,
    rows_ref,
    meta_ref,
    meta,
    mix_ref,
    cluster,
    near_src,
    near_tgt,
    near_mix,
    near_out,
    sent,
    got,
    lhs,
    acc,
    comp_got,
    total,
    cast,
    src_got,
    load_sem,
    u_sem,
    meta_sem,
    send_sem,
    recv_sem,
    comp_send,
    comp_recv,
    src_send,
    src_recv,
):
    groups, shards, pairing, components, chunk = sizes
    me = lax.axis_index("tgt")
    row = lax.axis_index("src")
    half_of = lax.axis_index("comp")
    owned, channels, size = x_ref.shape
    vectors = channels // components
    strip = vectors // HALVES
    band = components * strip
    slots, rank_width = u_hbm.shape[0] * 2, u_hbm.shape[1] // 2
    blocks = v_hbm.shape[0]
    capacity = slots // groups
    pairs = capacity // 2
    lanes = 2 * rank_width
    chunks = pairs // chunk
    targets = acc.shape[1] // band
    kept = targets // (pairing * shards)

    def load(index, source, target):
        return pltpu.make_async_copy(source, target, load_sem.at[index])

    small = [
        load(0, dest_hbm, rows_ref.at[0]),
        load(1, ranks_hbm, rows_ref.at[1]),
        load(2, src_hbm, rows_ref.at[2]),
    ]
    early = [load(3, field_hbm, field_ref), load(4, mix_hbm, mix_ref)]
    later = [
        load(9, near_hbm, near_ref),
        load(10, cluster_hbm, cluster),
        load(11, near_src_hbm, near_src),
        load(12, near_tgt_hbm, near_tgt),
        load(13, near_mix_hbm, near_mix),
    ]
    split = 4 if blocks % 4 == 0 else 1
    part = blocks // split
    v_loads = [
        load(5 + i, v_hbm.at[pl.ds(i * part, part)], v_ref.at[pl.ds(i * part, part)])
        for i in range(split)
    ]
    u_loads = [
        pltpu.make_async_copy(
            u_hbm.at[pl.ds(g * pairs, pairs)], u_ref.at[pl.ds(g * pairs, pairs)], u_sem.at[g]
        )
        for g in range(groups)
    ]
    for copy in small + early + v_loads:
        copy.start()

    barrier = pltpu.get_barrier_semaphore()
    for step in range(1, groups):
        pl.semaphore_signal(
            barrier, inc=1, device_id={"tgt": jnp.bitwise_xor(me, step)}, device_id_type=MESH
        )
    for step in range(1, shards):
        pl.semaphore_signal(
            barrier, inc=1, device_id={"src": lax.rem(row + step, shards)}, device_id_type=MESH
        )
    for step in range(1, pairing):
        pl.semaphore_signal(
            barrier, inc=1, device_id={"comp": lax.rem(half_of + step, pairing)}, device_id_type=MESH
        )

    for copy in small:
        copy.wait()
    dest = rows_ref[0]
    padded = -(-groups // 16) * 16
    member = jnp.where(
        lax.broadcasted_iota(jnp.int32, (padded, blocks), 0) == dest, 1.0, 0.0
    )
    before = jnp.where(
        lax.broadcasted_iota(jnp.int32, (blocks, blocks), 0)
        < lax.broadcasted_iota(jnp.int32, (blocks, blocks), 1),
        1.0,
        0.0,
    ).astype(jnp.bfloat16)
    earlier = jnp.dot(member.astype(jnp.bfloat16), before, preferred_element_type=jnp.float32)
    position = jnp.sum(member * earlier, axis=0, keepdims=True)
    slot = dest * capacity + position.astype(jnp.int32)
    taken = jnp.where(
        lax.broadcasted_iota(jnp.int32, (slots, blocks), 0) == slot, 1.0, 0.0
    ).astype(jnp.bfloat16)
    line = lax.broadcasted_iota(jnp.int32, (16, blocks), 0)
    facts = jnp.where(
        line == 0,
        lax.broadcasted_iota(jnp.int32, (16, blocks), 1),
        jnp.where(line == 1, rows_ref[1], rows_ref[2]),
    )
    placed = lax.dot_general(
        facts.astype(jnp.float32).astype(jnp.bfloat16), taken, NT, preferred_element_type=jnp.float32
    )
    meta_ref[...] = placed[:8].astype(jnp.int32)
    to_scalars = pltpu.make_async_copy(meta_ref, meta, meta_sem)
    to_scalars.start()

    early[0].wait()
    for s in range(owned):
        x_ref[s] = field_ref[:, s * size : (s + 1) * size]
    to_scalars.wait()
    for copy in early[1:] + v_loads:
        copy.wait()
    for copy in later + u_loads:
        copy.start()

    lane = lax.broadcasted_iota(jnp.int32, (1, lanes), 1)
    first = lane < rank_width
    rank_at = lane % rank_width
    unroll = 4 if chunk % 4 == 0 else 1

    def coef_step(offset, start):
        base = jnp.bitwise_xor(me, offset) * capacity + 2 * start
        numbers = [jnp.clip(meta[0, base + i], 0, blocks - 1) for i in range(2 * unroll)]
        v = jnp.concatenate([v_ref[b] for b in numbers], axis=0)
        x = x_ref[...].reshape(owned * channels, size)
        y = lax.dot_general(x, v, NT, preferred_element_type=jnp.float32)
        for u in range(unroll):
            b0, b1 = numbers[2 * u], numbers[2 * u + 1]
            k0, k1 = base + 2 * u, base + 2 * u + 1
            here = y[:, u * lanes : (u + 1) * lanes]
            chosen = jnp.where(first, meta[2, k0], meta[2, k1])
            coef = here[:channels]
            for s in range(1, owned):
                coef = jnp.where(chosen == s, here[s * channels : (s + 1) * channels], coef)
            coef = jnp.where(rank_at < jnp.where(first, meta[1, k0], meta[1, k1]), coef, 0.0)
            weights = [
                [jnp.where(first, mix_ref[c, d, b0], mix_ref[c, d, b1]) for d in range(components)]
                for c in range(components)
            ]
            mixed = mix_rows(
                weights, [coef[d * vectors : (d + 1) * vectors] for d in range(components)]
            )
            for h in range(HALVES):
                for c in range(components):
                    sent[offset, h, start + u, c * strip : (c + 1) * strip, :] = mixed[c][
                        h * strip : (h + 1) * strip
                    ].astype(jnp.bfloat16)

    def coef_chunk(offset, c):
        def several(step, carry):
            coef_step(offset, c * chunk + step * unroll)
            return carry

        lax.fori_loop(0, chunk // unroll, several, 0)

    def exchange(offset, h, c):
        where = (h, pl.ds(c * chunk, chunk))
        return pltpu.make_async_remote_copy(
            src_ref=sent.at[(offset,) + where],
            dst_ref=got.at[(offset - 1,) + where],
            send_sem=send_sem.at[h, offset - 1, c],
            recv_sem=recv_sem.at[h, offset - 1, c],
            device_id={"tgt": jnp.bitwise_xor(me, offset)},
            device_id_type=MESH,
        )

    def over_offsets(action):
        def step(t, carry):
            action(groups - 1 - t)
            return carry

        lax.fori_loop(0, groups - 1, step, 0)

    def over_chunks(action):
        def step(c, carry):
            action(c)
            return carry

        lax.fori_loop(0, chunks, step, 0)

    pl.semaphore_wait(barrier, groups + shards + pairing - 3)

    def send_first(c):
        def one(offset):
            coef_chunk(offset, c)
            exchange(offset, 0, c).start()

        over_offsets(one)

    over_chunks(send_first)
    for h in range(1, HALVES):
        over_chunks(lambda c, h=h: over_offsets(lambda offset: exchange(offset, h, c).start()))
    over_chunks(lambda c: coef_chunk(0, c))

    for copy in later:
        copy.wait()
    for n in range(near_ref.shape[0]):
        y = lax.dot_general(
            x_ref[near_src[n]], near_ref[n], NT, preferred_element_type=jnp.float32
        )
        weights = [[near_mix[c, n, d] for d in range(components)] for c in range(components)]
        mixed = mix_rows(weights, [y[d * vectors : (d + 1) * vectors] for d in range(components)])
        for h in range(HALVES):
            for c in range(components):
                near_out[h, n, c * strip : (c + 1) * strip, :] = mixed[c][
                    h * strip : (h + 1) * strip
                ]

    def place_near(w, carry):
        for h in range(HALVES):
            value = jnp.where(near_tgt[0] == w, near_out[h, 0], 0.0)
            for n in range(1, near_ref.shape[0]):
                value = value + jnp.where(near_tgt[n] == w, near_out[h, n], 0.0)
            acc[h, pl.ds(pl.multiple_of(w * band, band), band), :] = value
        return carry

    lax.fori_loop(0, targets, place_near, 0)
    for copy in u_loads:
        copy.wait()

    wide_first = lax.broadcasted_iota(jnp.int32, (strip, lanes), 1) < rank_width

    def far(h, offset, c, read):
        base = jnp.bitwise_xor(me, offset) * pairs + c * chunk
        for u in range(chunk):
            ids = jnp.where(wide_first, cluster[2 * (base + u)], cluster[2 * (base + u) + 1])
            value = read(c * chunk + u)
            for w in range(targets):
                on = jnp.where(ids == w, 1.0, 0.0).astype(jnp.bfloat16)
                for c3 in range(components):
                    lhs[pl.ds(w * band + c3 * strip, strip), u * lanes : (u + 1) * lanes] = (
                        value[c3 * strip : (c3 + 1) * strip] * on
                    )
        basis = u_ref[pl.ds(base, chunk)].reshape(chunk * lanes, size)
        acc[h] += jnp.dot(lhs[...], basis, preferred_element_type=jnp.float32)

    def far_own(h):
        over_chunks(lambda c: far(h, 0, c, lambda m: sent[0, h, m]))

    def far_chunk(h, c):
        def one(offset):
            exchange(offset, h, c).wait_recv()
            far(h, offset, c, lambda m: got[offset - 1, h, m])

        over_offsets(one)

    portion = shards * kept * band

    def comp_copy(h, step):
        to = lax.rem(half_of + step, pairing)
        return pltpu.make_async_remote_copy(
            src_ref=acc.at[h, pl.ds(pl.multiple_of(to * portion, portion), portion)],
            dst_ref=comp_got.at[h, step - 1],
            send_sem=comp_send.at[h, step - 1],
            recv_sem=comp_recv.at[h, step - 1],
            device_id={"comp": to},
            device_id_type=MESH,
        )

    piece = kept * band

    def src_copy(h, step):
        to = lax.rem(row + step, shards)
        return pltpu.make_async_remote_copy(
            src_ref=cast.at[h, pl.ds(pl.multiple_of(to * piece, piece), piece)],
            dst_ref=src_got.at[h, step - 1],
            send_sem=src_send.at[h, step - 1],
            recv_sem=src_recv.at[h, step - 1],
            device_id={"src": to},
            device_id_type=MESH,
        )

    def share_comp(h):
        for step in range(1, pairing):
            comp_copy(h, step).start()

    def share_src(h):
        for step in range(1, pairing):
            comp_copy(h, step).wait_recv()
        value = acc[h, pl.ds(pl.multiple_of(half_of * portion, portion), portion), :]
        for step in range(1, pairing):
            value = value + comp_got[h, step - 1]
        total[h] = value
        cast[h] = value.astype(jnp.bfloat16)
        for step in range(1, shards):
            src_copy(h, step).start()

    def finish(h):
        value = total[h, pl.ds(pl.multiple_of(row * piece, piece), piece), :]
        for step in range(1, shards):
            src_copy(h, step).wait_recv()
            value = value + src_got[h, step - 1].astype(jnp.float32)
        for k in range(kept):
            for c in range(components):
                at = k * band + c * strip
                out_ref[c, h * strip : (h + 1) * strip, k * size : (k + 1) * size] = value[
                    at : at + strip
                ]

    for h in range(HALVES):
        far_own(h)
    for h in range(HALVES):
        over_chunks(functools.partial(far_chunk, h))
        share_comp(h)
        share_src(h)
        if h:
            finish(h - 1)
    finish(HALVES - 1)

    for h in range(HALVES):
        over_chunks(lambda c, h=h: over_offsets(lambda offset: exchange(offset, h, c).wait_send()))
        for step in range(1, pairing):
            comp_copy(h, step).wait_send()
        for step in range(1, shards):
            src_copy(h, step).wait_send()


def packed_kernel(
    sizes,
    field_hbm,
    dest_hbm,
    src_hbm,
    ranks_hbm,
    mix_hbm,
    v_hbm,
    u_hbm,
    cluster_hbm,
    near_src_hbm,
    near_tgt_hbm,
    near_mix_hbm,
    near_hbm,
    out_ref,
    flag_ref,
    field_ref,
    x_ref,
    v_ref,
    u_ref,
    near_ref,
    rows_ref,
    meta_ref,
    meta,
    mix_ref,
    weight_ref,
    table_got,
    table,
    flag_row,
    flag_got,
    cluster,
    near_src,
    near_tgt,
    near_mix,
    near_out,
    sent,
    got,
    lhs,
    rhs,
    acc,
    comp_got,
    total,
    cast,
    src_got,
    load_sem,
    u_sem,
    meta_sem,
    send_sem,
    recv_sem,
    comp_send,
    comp_recv,
    src_send,
    src_recv,
    table_send,
    table_recv,
    table_sem,
    flag_send,
    flag_recv,
):
    groups, shards, pairing, components, limit, plan = sizes
    me = lax.axis_index("tgt")
    row = lax.axis_index("src")
    half_of = lax.axis_index("comp")
    owned, channels, size = x_ref.shape
    vectors = channels // components
    strip = vectors // HALVES
    band = components * strip
    lanes = sent.shape[-1]
    tiles_in = lanes // TILE
    whole = sent.shape[2]
    full = whole * tiles_in
    blocks = weight_ref.shape[0]
    tiles = v_hbm.shape[0]
    per_block = tiles // blocks
    capacity = full // per_block
    targets = acc.shape[1] // band
    kept = targets // (pairing * shards)

    def load(index, source, target):
        return pltpu.make_async_copy(source, target, load_sem.at[index])

    small = [
        load(0, dest_hbm, rows_ref.at[0]),
        load(1, ranks_hbm, rows_ref.at[1]),
        load(2, src_hbm, rows_ref.at[2]),
    ]
    early = [load(3, field_hbm, field_ref), load(4, mix_hbm, mix_ref)]
    later = [
        load(9, near_hbm, near_ref),
        load(10, cluster_hbm, cluster),
        load(11, near_src_hbm, near_src),
        load(12, near_tgt_hbm, near_tgt),
        load(13, near_mix_hbm, near_mix),
    ]
    split = 4 if tiles % 4 == 0 else 1
    part = tiles // split
    v_loads = [
        load(5 + i, v_hbm.at[pl.ds(i * part, part)], v_ref.at[pl.ds(i * part, part)])
        for i in range(split)
    ]
    u_loads = [
        pltpu.make_async_copy(
            u_hbm.at[pl.ds(g * full, full)], u_ref.at[pl.ds(g * full, full)], u_sem.at[g]
        )
        for g in range(groups)
    ]
    for copy in small + early + v_loads:
        copy.start()

    barrier = pltpu.get_barrier_semaphore()
    for step in range(1, groups):
        pl.semaphore_signal(
            barrier, inc=1, device_id={"tgt": jnp.bitwise_xor(me, step)}, device_id_type=MESH
        )
    for step in range(1, shards):
        pl.semaphore_signal(
            barrier, inc=1, device_id={"src": lax.rem(row + step, shards)}, device_id_type=MESH
        )
    for step in range(1, pairing):
        pl.semaphore_signal(
            barrier, inc=1, device_id={"comp": lax.rem(half_of + step, pairing)}, device_id_type=MESH
        )

    for copy in small:
        copy.wait()
    dest, rank, source = rows_ref[0], rows_ref[1], rows_ref[2]
    count = lax.shift_right_logical(rank + (TILE - 1), TILE_BITS)
    padded = -(-groups // 16) * 16
    group_at = lax.broadcasted_iota(jnp.int32, (padded, blocks), 0)
    member = jnp.where(group_at == dest, 1.0, 0.0)
    both = jnp.concatenate([member, member * count.astype(jnp.float32)], axis=0)
    before = jnp.where(
        lax.broadcasted_iota(jnp.int32, (blocks, blocks), 0)
        < lax.broadcasted_iota(jnp.int32, (blocks, blocks), 1),
        1.0,
        0.0,
    ).astype(jnp.bfloat16)
    earlier = jnp.dot(both.astype(jnp.bfloat16), before, preferred_element_type=jnp.float32)
    position = jnp.sum(member * earlier[:padded], axis=0, keepdims=True).astype(jnp.int32)
    tile_at = jnp.sum(member * earlier[padded:], axis=0, keepdims=True).astype(jnp.int32)
    used = jnp.sum(both[padded:], axis=1, keepdims=True)
    away = lax.broadcasted_iota(jnp.int32, (padded, 1), 0) != me
    most = jnp.max(jnp.where(away, used, 0.0), axis=0, keepdims=True)
    over = jnp.where(most > float(limit * tiles_in), 1, 0)
    start = dest * full + tile_at
    ahead = lax.broadcasted_iota(jnp.int32, (groups * full, blocks), 0) - start
    taken = jnp.where((ahead >= 0) & (ahead < count), 1.0, 0.0).astype(jnp.bfloat16)
    line = lax.broadcasted_iota(jnp.int32, (16, blocks), 0)
    facts = jnp.where(line == 0, lax.broadcasted_iota(jnp.int32, (16, blocks), 1), 1)
    for at, fact in enumerate((rank, source, position, tile_at)):
        facts = jnp.where(line == at + 1, fact, facts)
    placed = lax.dot_general(
        facts.astype(jnp.float32).astype(jnp.bfloat16), taken, NT, preferred_element_type=jnp.float32
    )
    placed = placed.astype(jnp.int32)
    where_at = lax.broadcasted_iota(jnp.int32, (1, groups * full), 1) % full
    sub = jnp.where(placed[5:6] > 0, where_at - placed[4:5], 0)
    table_rows = [
        placed[0:1] * per_block + sub,
        placed[0:1],
        placed[2:3],
        jnp.clip(placed[1:2] - TILE * sub, 0, TILE),
        placed[3:4] * per_block + sub,
        jnp.broadcast_to(over, (1, groups * full)),
    ]
    table_rows = jnp.concatenate(table_rows + table_rows[-1:] * 2, axis=0)
    for g in range(groups):
        meta_ref[g] = table_rows[:, g * full : (g + 1) * full]
    to_scalars = pltpu.make_async_copy(meta_ref, meta, meta_sem)
    to_scalars.start()

    early[1].wait()
    entries = [mix_ref[c, d : d + 1, :] for c in range(components) for d in range(components)]
    entries = jnp.concatenate(entries + entries[:1] * (16 - len(entries)), axis=0)
    for b in range(blocks):
        weight_ref[b] = jnp.broadcast_to(entries[:, b : b + 1], (16, lanes))

    early[0].wait()
    for s in range(owned):
        x_ref[s] = field_ref[:, s * size : (s + 1) * size]
    to_scalars.wait()
    for copy in v_loads:
        copy.wait()
    for copy in later + u_loads:
        copy.start()

    lane = lax.broadcasted_iota(jnp.int32, (1, lanes), 1)
    in_tile = lane % TILE
    tile_of = lane // TILE

    def spread(values):
        vector = values[0]
        for i, value in enumerate(values[1:]):
            vector = jnp.where(tile_of == i + 1, value, vector)
        return vector

    def coef_step(offset, start, unroll):
        to = jnp.bitwise_xor(me, offset)

        def entry(fact, u, i):
            return meta[to, fact, (start + u) * tiles_in + i]

        v = jnp.concatenate(
            [
                v_ref[jnp.clip(entry(0, u, i), 0, tiles - 1)]
                for u in range(unroll)
                for i in range(tiles_in)
            ],
            axis=0,
        )
        x = x_ref[...].reshape(owned * channels, size)
        y = lax.dot_general(x, v, NT, preferred_element_type=jnp.float32)
        for u in range(unroll):
            here = y[:, u * lanes : (u + 1) * lanes]
            chosen = spread([entry(2, u, i) for i in range(tiles_in)])
            coef = here[:channels]
            for s in range(1, owned):
                coef = jnp.where(chosen == s, here[s * channels : (s + 1) * channels], coef)
            coef = jnp.where(in_tile < spread([entry(3, u, i) for i in range(tiles_in)]), coef, 0.0)
            weight = spread(
                [weight_ref[jnp.clip(entry(1, u, i), 0, blocks - 1)] for i in range(tiles_in)]
            )
            weights = [
                [weight[c * components + d : c * components + d + 1] for d in range(components)]
                for c in range(components)
            ]
            mixed = mix_rows(
                weights, [coef[d * vectors : (d + 1) * vectors] for d in range(components)]
            )
            for h in range(HALVES):
                for c in range(components):
                    sent[offset, h, start + u, c * strip : (c + 1) * strip, :] = mixed[c][
                        h * strip : (h + 1) * strip
                    ].astype(jnp.bfloat16)

    def coef_chunk(offset, begin, length):
        unroll = next(u for u in (4, 3, 2, 1) if length % u == 0)

        def several(step, carry):
            coef_step(offset, begin + step * unroll, unroll)
            return carry

        lax.fori_loop(0, length // unroll, several, 0)

    def exchange(offset, h, c):
        where = (h, pl.ds(*plan[c]))
        return pltpu.make_async_remote_copy(
            src_ref=sent.at[(offset,) + where],
            dst_ref=got.at[(offset - 1,) + where],
            send_sem=send_sem.at[h, offset - 1, c],
            recv_sem=recv_sem.at[h, offset - 1, c],
            device_id={"tgt": jnp.bitwise_xor(me, offset)},
            device_id_type=MESH,
        )

    def over_offsets(action):
        def step(t, carry):
            action(groups - 1 - t)
            return carry

        lax.fori_loop(0, groups - 1, step, 0)

    def table_copy(offset):
        to = jnp.bitwise_xor(me, offset)
        return pltpu.make_async_remote_copy(
            src_ref=meta_ref.at[to],
            dst_ref=table_got.at[offset - 1],
            send_sem=table_send.at[offset - 1],
            recv_sem=table_recv.at[offset - 1],
            device_id={"tgt": to},
            device_id_type=MESH,
        )

    def table_down(offset):
        return pltpu.make_async_copy(
            table_got.at[offset - 1], table.at[offset - 1], table_sem.at[offset - 1]
        )

    pl.semaphore_wait(barrier, groups + shards + pairing - 3)
    over_offsets(lambda offset: table_copy(offset).start())
    for c, (begin, length) in enumerate(plan):

        def one(offset):
            coef_chunk(offset, begin, length)
            exchange(offset, 0, c).start()

        over_offsets(one)
    for h in range(1, HALVES):
        for c in range(len(plan)):
            over_offsets(lambda offset: exchange(offset, h, c).start())
    coef_chunk(0, 0, whole)

    def fetch(offset):
        table_copy(offset).wait_recv()
        table_down(offset).start()

    over_offsets(fetch)
    for copy in later:
        copy.wait()
    for n in range(near_ref.shape[0]):
        y = lax.dot_general(
            x_ref[near_src[n]], near_ref[n], NT, preferred_element_type=jnp.float32
        )
        weights = [[near_mix[c, n, d] for d in range(components)] for c in range(components)]
        mixed = mix_rows(weights, [y[d * vectors : (d + 1) * vectors] for d in range(components)])
        for h in range(HALVES):
            for c in range(components):
                near_out[h, n, c * strip : (c + 1) * strip, :] = mixed[c][
                    h * strip : (h + 1) * strip
                ]

    def place_near(w, carry):
        for h in range(HALVES):
            value = jnp.where(near_tgt[0] == w, near_out[h, 0], 0.0)
            for n in range(1, near_ref.shape[0]):
                value = value + jnp.where(near_tgt[n] == w, near_out[h, n], 0.0)
            acc[h, pl.ds(pl.multiple_of(w * band, band), band), :] = value
        return carry

    lax.fori_loop(0, targets, place_near, 0)
    for copy in u_loads:
        copy.wait()

    wide_tile = lax.broadcasted_iota(jnp.int32, (strip, lanes), 1) // TILE

    def build(n, sender, entry, begin, length, read):
        for u in range(length):
            ids = None
            for i in range(tiles_in):
                at = jnp.clip(entry((begin + u) * tiles_in + i), 0, full - 1)
                rhs[n, u * lanes + i * TILE : u * lanes + (i + 1) * TILE, :] = u_ref[
                    sender * full + at
                ]
                target = cluster[sender * capacity + lax.div(at, per_block)]
                ids = jnp.full((strip, lanes), target) if i == 0 else jnp.where(wide_tile == i, target, ids)
            value = read(begin + u)
            for w in range(targets):
                on = jnp.where(ids == w, 1.0, 0.0).astype(jnp.bfloat16)
                for c3 in range(components):
                    lhs[n, pl.ds(w * band + c3 * strip, strip), u * lanes : (u + 1) * lanes] = (
                        value[c3 * strip : (c3 + 1) * strip] * on
                    )

    def multiply(h, n, length):
        acc[h] += jnp.dot(
            lhs[n, :, : length * lanes], rhs[n, : length * lanes], preferred_element_type=jnp.float32
        )

    def far(h, work):
        build(0, *work[0])
        for n in range(1, len(work)):
            build(n, *work[n])
            multiply(h, n - 1, work[n - 1][3])
        multiply(h, len(work) - 1, work[-1][3])

    batch = 3 if (groups - 1) % 3 == 0 else 1

    def far_own(h):
        block = 8 if whole % 8 == 0 else 1
        many = 2 if (whole // block) % 2 == 0 and batch > 1 else 1

        def several(c, carry):
            far(
                h,
                [
                    (me, lambda t: meta[me, 4, t], (c * many + n) * block, block, lambda m: sent[0, h, m])
                    for n in range(many)
                ],
            )
            return carry

        lax.fori_loop(0, whole // block // many, several, 0)

    def far_chunk(h, c):
        def several(t, carry):
            offsets = [groups - 1 - (t * batch + n) for n in range(batch)]
            for offset in offsets:
                exchange(offset, h, c).wait_recv()
            far(
                h,
                [
                    (
                        jnp.bitwise_xor(me, offset),
                        lambda t, offset=offset: table[offset - 1, 4, t],
                        *plan[c],
                        lambda m, offset=offset: got[offset - 1, h, m],
                    )
                    for offset in offsets
                ],
            )
            return carry

        if groups - 1 == batch:
            several(0, 0)
        else:
            lax.fori_loop(0, (groups - 1) // batch, several, 0)

    def flag_copy(step):
        axis, place, span, by = (
            ("comp", half_of, pairing, step) if step < pairing else ("src", row, shards, step - pairing + 1)
        )
        kind = 0 if axis == "comp" else 1
        return pltpu.make_async_remote_copy(
            src_ref=flag_row.at[kind],
            dst_ref=flag_got.at[step - 1],
            send_sem=flag_send.at[step - 1],
            recv_sem=flag_recv.at[step - 1],
            device_id={axis: lax.rem(place + by, span)},
            device_id_type=MESH,
        )

    comp_steps = range(1, pairing)
    src_steps = range(pairing, pairing + shards - 1)

    portion = shards * kept * band

    piece = kept * band
    power = shards & (shards - 1) == 0

    def peer(step):
        return jnp.bitwise_xor(row, step) if power else lax.rem(row + step, shards)

    hops = list(range(shards - 1, -1, -1))

    def comp_copy(h, step, hop):
        to = lax.rem(half_of + step, pairing)
        which = pl.multiple_of(peer(hop) * piece, piece)
        return pltpu.make_async_remote_copy(
            src_ref=acc.at[h, pl.ds(pl.multiple_of(to * portion, portion) + which, piece)],
            dst_ref=comp_got.at[h, step - 1, pl.ds(which, piece)],
            send_sem=comp_send.at[h, step - 1, hop],
            recv_sem=comp_recv.at[h, step - 1, hop],
            device_id={"comp": to},
            device_id_type=MESH,
        )

    def src_copy(h, step):
        to = peer(step)
        return pltpu.make_async_remote_copy(
            src_ref=cast.at[h, pl.ds(pl.multiple_of(to * piece, piece), piece)],
            dst_ref=src_got.at[h, step - 1],
            send_sem=src_send.at[h, step - 1],
            recv_sem=src_recv.at[h, step - 1],
            device_id={"src": to},
            device_id_type=MESH,
        )

    def share_comp(h):
        for hop in hops:
            for step in range(1, pairing):
                comp_copy(h, step, hop).start()

    def share_src(h):
        mine = pl.multiple_of(half_of * portion, portion)
        for hop in hops:
            which = pl.multiple_of(peer(hop) * piece, piece)
            value = acc[h, pl.ds(mine + which, piece), :]
            for step in range(1, pairing):
                comp_copy(h, step, hop).wait_recv()
                value = value + comp_got[h, step - 1, pl.ds(which, piece), :]
            if hop:
                cast[h, pl.ds(which, piece), :] = value.astype(jnp.bfloat16)
                src_copy(h, hop).start()
            else:
                total[h, pl.ds(which, piece), :] = value

    def finish(h):
        value = total[h, pl.ds(pl.multiple_of(row * piece, piece), piece), :]
        for step in range(1, shards):
            src_copy(h, step).wait_recv()
            value = value + src_got[h, step - 1].astype(jnp.float32)
        for k in range(kept):
            for c in range(components):
                at = k * band + c * strip
                out_ref[c, h * strip : (h + 1) * strip, k * size : (k + 1) * size] = value[
                    at : at + strip
                ]

    seen = over
    for offset in range(1, groups):
        seen = jnp.maximum(seen, table_got[offset - 1, 5:6, 0:1])
        table_down(offset).wait()
    flag_row[0] = jnp.broadcast_to(seen, flag_row.shape[1:])
    for step in comp_steps:
        flag_copy(step).start()
    far_own(0)
    seen = flag_row[0]
    for step in comp_steps:
        flag_copy(step).wait_recv()
        seen = jnp.maximum(seen, flag_got[step - 1])
    flag_row[1] = seen
    for step in src_steps:
        flag_copy(step).start()
    for h in range(1, HALVES):
        far_own(h)
    seen = flag_row[1]
    for step in src_steps:
        flag_copy(step).wait_recv()
        seen = jnp.maximum(seen, flag_got[step - 1])
    flag_ref[...] = seen
    for h in range(HALVES):
        for c in range(len(plan)):
            far_chunk(h, c)
        share_comp(h)
        share_src(h)
        if h:
            finish(h - 1)
    finish(HALVES - 1)

    over_offsets(lambda offset: table_copy(offset).wait_send())
    for step in list(comp_steps) + list(src_steps):
        flag_copy(step).wait_send()
    for h in range(HALVES):
        for c in range(len(plan)):
            over_offsets(lambda offset: exchange(offset, h, c).wait_send())
        for step in range(1, pairing):
            for hop in hops:
                comp_copy(h, step, hop).wait_send()
        for step in range(1, shards):
            src_copy(h, step).wait_send()


def body(
    field,
    dest_group,
    src_local,
    ranks,
    mixing,
    v_factor,
    u_factor,
    slot_cluster,
    near_src,
    near_tgt,
    near_mixing,
    near_matrix,
):
    groups = lax.axis_size("tgt")
    shards = lax.axis_size("src")
    pairing = lax.axis_size("comp")
    blocks, rank_width, size = v_factor.shape
    components, vectors, points = field.shape
    channels = components * vectors
    owned = points // size
    slots = u_factor.shape[0]
    pairs = slots // groups // 2
    targets = owned * shards
    kept = targets // (pairing * shards)
    lanes = 2 * rank_width
    band = channels // HALVES
    near_count = near_matrix.shape[0]
    portion = shards * kept * band
    f32, bf16, i32 = jnp.float32, jnp.bfloat16, jnp.int32
    dma = pltpu.SemaphoreType.DMA
    result = pltpu.VMEM((components, vectors, kept * size), f32)
    inputs = (
        field.reshape(channels, points),
        dest_group.reshape(1, -1),
        src_local.reshape(1, -1),
        ranks.reshape(1, -1),
        mixing.transpose(1, 2, 0),
    )
    near_inputs = (
        slot_cluster,
        near_src,
        near_tgt,
        near_mixing.transpose(1, 0, 2),
        near_matrix,
    )
    near_scalars = [
        pltpu.SMEM((slots,), i32),
        pltpu.SMEM((near_count,), i32),
        pltpu.SMEM((near_count,), i32),
        pltpu.SMEM((components, near_count, components), f32),
        pltpu.VMEM((HALVES, near_count, band, size), f32),
    ]
    reduce_buffers = [
        pltpu.VMEM((HALVES, targets * band, size), f32),
        pltpu.VMEM((HALVES, pairing - 1, portion, size), f32),
        pltpu.VMEM((HALVES, portion, size), f32),
        pltpu.VMEM((HALVES, portion, size), bf16),
        pltpu.VMEM((HALVES, shards - 1, kept * band, size), bf16),
        dma((14,)),
        dma((groups,)),
        dma,
    ]
    reduce_sems = [
        dma((HALVES, pairing - 1)),
        dma((HALVES, pairing - 1)),
        dma((HALVES, shards - 1)),
        dma((HALVES, shards - 1)),
    ]
    field_buffers = [
        pltpu.VMEM((channels, points), bf16),
        pltpu.VMEM((owned, channels, size), bf16),
    ]

    def padded():
        chunk = 8 if pairs % 8 == 0 else pairs
        return pl.pallas_call(
            functools.partial(fused_kernel, (groups, shards, pairing, components, chunk)),
            out_shape=result,
            in_specs=[pl.BlockSpec(memory_space=pl.ANY)] * 12,
            out_specs=pl.BlockSpec(memory_space=pltpu.VMEM),
            scratch_shapes=field_buffers
            + [
                pltpu.VMEM((blocks, rank_width, size), bf16),
                pltpu.VMEM((slots // 2, lanes, size), bf16),
                pltpu.VMEM((near_count, size, size), bf16),
                pltpu.VMEM((3, 1, blocks), i32),
                pltpu.VMEM((8, slots), i32),
                pltpu.SMEM((8, slots), i32),
                pltpu.SMEM((components, components, blocks), f32),
            ]
            + near_scalars
            + [
                pltpu.VMEM((groups, HALVES, pairs, band, lanes), bf16),
                pltpu.VMEM((groups - 1, HALVES, pairs, band, lanes), bf16),
                pltpu.VMEM((targets * band, chunk * lanes), bf16),
            ]
            + reduce_buffers
            + [dma((HALVES, groups - 1, pairs // chunk))] * 2
            + reduce_sems,
            compiler_params=pltpu.CompilerParams(collective_id=1, has_side_effects=True),
            name="padded",
        )(*inputs, v_factor, u_factor.reshape(slots // 2, lanes, size), *near_inputs)

    per_block = rank_width // TILE
    tiles_in = lanes // TILE
    full = slots // groups * per_block
    whole = full // tiles_in
    share = 0.65 + (slots // groups) ** -0.5
    limit = min(whole, math.ceil(whole * share))
    plan = cut(limit)
    value, flag = pl.pallas_call(
        functools.partial(packed_kernel, (groups, shards, pairing, components, limit, plan)),
        out_shape=(result, pltpu.VMEM((8, lanes), i32)),
        in_specs=[pl.BlockSpec(memory_space=pl.ANY)] * 12,
        out_specs=(pl.BlockSpec(memory_space=pltpu.VMEM),) * 2,
        scratch_shapes=field_buffers
        + [
            pltpu.VMEM((blocks * per_block, TILE, size), bf16),
            pltpu.VMEM((slots * per_block, TILE, size), bf16),
            pltpu.VMEM((near_count, size, size), bf16),
            pltpu.VMEM((3, 1, blocks), i32),
            pltpu.VMEM((groups, 8, full), i32),
            pltpu.SMEM((groups, 8, full), i32),
            pltpu.VMEM((components, components, blocks), f32),
            pltpu.VMEM((blocks, 16, lanes), f32),
            pltpu.VMEM((groups - 1, 8, full), i32),
            pltpu.SMEM((groups - 1, 8, full), i32),
            pltpu.VMEM((2, 8, lanes), i32),
            pltpu.VMEM((pairing + shards - 2, 8, lanes), i32),
        ]
        + near_scalars
        + [
            pltpu.VMEM((groups, HALVES, whole, band, lanes), bf16),
            pltpu.VMEM((groups - 1, HALVES, limit, band, lanes), bf16),
            pltpu.VMEM((3, targets * band, 8 * lanes), bf16),
            pltpu.VMEM((3, 8 * lanes, size), bf16),
        ]
        + reduce_buffers
        + [dma((HALVES, groups - 1, len(plan)))] * 2
        + [dma((HALVES, pairing - 1, shards))] * 2
        + reduce_sems[2:]
        + [dma((groups - 1,))] * 3
        + [dma((pairing + shards - 2,))] * 2,
        compiler_params=pltpu.CompilerParams(collective_id=0, has_side_effects=True),
        name="packed",
    )(
        *inputs,
        v_factor.reshape(blocks * per_block, TILE, size),
        u_factor.reshape(slots * per_block, TILE, size),
        *near_inputs,
    )
    if limit == whole:
        return value
    return lax.cond(flag[0, 0] > 0, padded, lambda: value)


def solution(mesh):
    everywhere = ("comp", "tgt", "src")
    placed = (
        P(None, None, ("tgt", "src")),
        P(everywhere, None),
        P(everywhere),
        P(everywhere),
        P(everywhere, None, None),
        P(everywhere, None, None),
        P(everywhere, None, None),
        P(everywhere),
        P(everywhere),
        P(everywhere),
        P(everywhere, None, None),
        P(everywhere, None, None),
    )
    return jax.shard_map(
        body,
        mesh=mesh,
        in_specs=placed,
        out_specs=P(None, None, everywhere),
        check_vma=False,
    )
```
